128 devices in a mesh: zm: 16 (over y, x), zv: 8 (over z, core).
Axes of the slice: x: 4, y: 4, z: 4, core: 2. Of those that a mesh axis runs over, the one named last changes fastest.
Arguments:
- table: float32 [256, 512, 256], P('zm', 'zv'), may hold values from -6 to 6
- refined: float32 [4, 2048, 16, 1024], P(None, ('zm', 'zv')), may hold values from -18 to 18
- assign: int32 [4, 128, 16], replicated, may hold values from -1 to 2047, as said below
Outputs:
- table_out: float32 [256, 512, 256], P('zm', 'zv')
- block_error: float32 [4, 2048], P(None, ('zm', 'zv'))
- worst: float32 [4], replicated
The draws below stay inside these ranges and needn't reach their ends.
Inputs may be any that keep to these rules, and one draw needn't show every extreme that they name: `assign`: devices are numbered d = zm index * 8 + zv index; block b is homed on device b // 16, and its home device has the same zv index as the owner d of the slot. In an iteration no block appears twice, at most 1 block of one home device sit in the slots of one owner (reached in every iteration), and some owner of every zv index has all 16 slots filled.
All inputs are finite; a program needn't handle non-finite values.
Results may differ from the reference program's by a relative error of at most 0.0001.
Values sent between devices are 32-bit elements; how exact they have to be, the bound alone decides.
A program may use at most 128 MiB of HBM per device.

```python
import jax
import jax.numpy as jnp
from jax import lax

S = 8
NC = 32
BLOCK_Z = 16
BLOCK_V = 16
BLOCK_C = 8
ITERS = 4
CAP = 1
SLOTS = 16
NZ = 256
NV = 512
BLK_DEV = 16
SLOTS_ALL = 2048
N_ZM = 16
N_ZV = 8


def draw_assign(key, part):
    planes = []
    for iteration in range(ITERS):
        step_key = jax.random.fold_in(key, 101 + iteration)
        first_key, second_key, third_key, fourth_key = jax.random.split(step_key, 4)
        home_order = jax.vmap(lambda inner: jax.random.permutation(inner, N_ZM))(jax.random.split(first_key, N_ZV))
        picks = jax.vmap(lambda inner: jax.random.permutation(inner, BLK_DEV))(jax.random.split(second_key, N_ZV * N_ZM))
        picks = picks.reshape(N_ZV, N_ZM, BLK_DEV)
        owner_index = jnp.arange(N_ZM)[:, None, None]
        column_index = jnp.arange(N_ZV)[None, :, None]
        slot_index = jnp.arange(SLOTS)[None, None, :]
        position = (owner_index + slot_index // CAP) % N_ZM
        home_zm = home_order[column_index, position]
        local_id = picks[column_index, home_zm, owner_index * CAP + slot_index % CAP]
        full_owner = jax.random.randint(third_key, (1, N_ZV, 1), 0, N_ZM)
        coins = jax.random.randint(fourth_key, (N_ZM, N_ZV, SLOTS), 0, 2)
        live_mask = (coins == 1) | (owner_index == full_owner)
        block_ids = (home_zm * N_ZV + column_index) * BLK_DEV + local_id
        planes.append(jnp.where(live_mask, block_ids, -1).reshape(N_ZM * N_ZV, SLOTS))
    return jnp.stack(planes).astype(jnp.int32)


def draw_refined(key, part):
    shape_all = (ITERS, SLOTS_ALL, BLOCK_Z, BLOCK_V * BLOCK_C * S)
    inner_key = jax.random.fold_in(key, 7)
    base = jnp.clip(jax.random.normal(inner_key, shape_all, jnp.float32), -6.0, 6.0)
    owner_zm = jnp.arange(SLOTS_ALL) // SLOTS // N_ZV
    scale = 1.0 + 2.0 * owner_zm.astype(jnp.float32) / max(N_ZM - 1, 1)
    return base * scale[None, :, None, None]


def level_of(stream_key, dims, pieces, low, largest):
    loudness, own = 1.0, jax.random.fold_in(stream_key, 6)
    for dim, blocks in pieces:
        steps = jnp.exp(jax.random.uniform(jax.random.fold_in(own, dim), (blocks,), jnp.float32, low / len(pieces), largest / len(pieces)))
        loudness = loudness * jnp.repeat(steps, dims[dim] // blocks).reshape([-1 if axis == dim else 1 for axis in range(len(dims))])
    return loudness


def normal_values(key, extent, scale, limit, shards=(), held_as=jnp.bfloat16):
    values = scale * jax.random.normal(key, extent, jnp.float32)
    if shards:
        values = values * level_of(key, extent, shards, -0.22, 0.18)
    return jnp.clip(values, -limit, limit).astype(held_as)


def setup_inputs(seed: int = 0) -> dict:
    keys = jax.random.split(jax.random.key(seed), 4)
    return {
        "table": normal_values(keys[0], (NZ, NV, NC * S), 1.0, 6.0, ((0, 16), (1, 8)), jnp.float32),
        "refined": draw_refined(jax.random.fold_in(keys[3], 71), 0),
        "assign": draw_assign(jax.random.fold_in(keys[3], 71), 0),
    }


def corner_mean(corner_grid):
    summed = corner_grid[:-1, :-1, :-1] + corner_grid[1:, :-1, :-1] + corner_grid[:-1, 1:, :-1] + corner_grid[1:, 1:, :-1]
    summed = summed + corner_grid[:-1, :-1, 1:] + corner_grid[1:, :-1, 1:] + corner_grid[:-1, 1:, 1:] + corner_grid[1:, 1:, 1:]
    return summed * 0.125

def to_blocks(centre):
    size_z, size_v, size_c, size_s = centre.shape
    parts = centre.reshape(size_z // BLOCK_Z, BLOCK_Z, size_v // BLOCK_V, BLOCK_V, size_c // BLOCK_C, BLOCK_C, size_s)
    return parts.transpose(0, 2, 4, 1, 3, 5, 6).reshape(-1, BLOCK_Z * BLOCK_V * BLOCK_C * size_s)

def from_blocks(flat, size_z, size_v, size_c):
    parts = flat.reshape(size_z // BLOCK_Z, size_v // BLOCK_V, size_c // BLOCK_C, BLOCK_Z, BLOCK_V, BLOCK_C, S)
    return parts.transpose(0, 3, 1, 4, 2, 5, 6).reshape(size_z, size_v, size_c * S)

def reference(table, refined, assign):
    size_z, size_v, table_wide = table.shape
    size_c = table_wide // S
    block_cells = BLOCK_Z * BLOCK_V * BLOCK_C * S
    worst_list = []
    error_list = []
    for iteration in range(ITERS):
        corner_grid = table.reshape(size_z, size_v, size_c, S)
        corner_grid = jnp.concatenate([corner_grid, corner_grid[-1:]], 0)
        corner_grid = jnp.concatenate([corner_grid, corner_grid[:, -1:]], 1)
        corner_grid = jnp.concatenate([corner_grid, corner_grid[:, :, -1:]], 2)
        blocks = to_blocks(corner_mean(corner_grid))
        block_ids = assign[iteration].reshape(-1).astype(jnp.int32)
        live_mask = block_ids >= 0
        safe_ids = jnp.where(live_mask, block_ids, 0).astype(jnp.int32)
        target = refined[iteration].reshape(-1, block_cells)
        residual = jnp.where(live_mask[:, None], target - blocks[safe_ids], jnp.float32(0.0))
        total_sq = jnp.sum(residual * residual)
        cell_count = jnp.sum(live_mask.astype(jnp.float32)) * block_cells
        weight = 1.0 / (1.0 + jnp.sqrt(total_sq / cell_count))
        peak_error = lax.optimization_barrier(jnp.max(jnp.abs(residual), axis=1))
        worst_list.append(jnp.max(peak_error))
        errors = jnp.zeros((blocks.shape[0],), jnp.float32).at[safe_ids].max(jnp.where(live_mask, peak_error, jnp.float32(0.0)))
        error_list.append(errors)
        change = jnp.zeros_like(blocks).at[safe_ids].add(weight * residual)
        table = table + from_blocks(change, size_z, size_v, size_c)
    return (table, jnp.stack(error_list), jnp.stack(worst_list))
```

```python
import functools

import jax
import jax.numpy as jnp
from jax import lax
from jax.experimental import pallas as pl
from jax.experimental.pallas import tpu as pltpu
from jax.sharding import Mesh
from jax.sharding import PartitionSpec as P

ITERS = 4
Y, X, Z, C = "zm_0", "zm_1", "zv_0", "zv_1"
NAMES = (Y, X, Z, C)
ZM = (Y, X)
ZV = (Z, C)
BLK = 16
ROWS = 16
WIDE = 1024
META = 48
F32 = jnp.float32

ORDER = (
    (2, 2), (3, 2), (2, 3), (1, 2), (2, 1), (3, 1), (1, 3), (3, 3),
    (1, 1), (2, 0), (0, 2), (3, 0), (0, 3), (1, 0), (0, 1),
)
ZV_ORDER = ((2, 1), (2, 0), (1, 1), (3, 1), (1, 0), (3, 0), (0, 1))


def at(*steps):
    return tuple(
        lax.rem(lax.axis_index(name) + step + lax.axis_size(name), lax.axis_size(name))
        for name, step in zip(NAMES, steps, strict=True)
    )


def beside(zm_step, zv_step):
    zm = lax.rem(lax.axis_index(Y) * 4 + lax.axis_index(X) + zm_step + 16, 16)
    zv = lax.rem(lax.axis_index(Z) * 2 + lax.axis_index(C) + zv_step + 8, 8)
    return (zm // 4, lax.rem(zm, 4), zv // 2, lax.rem(zv, 2))


def send(src, dst, send_sem, recv_sem, device):
    copy = pltpu.make_async_remote_copy(
        src_ref=src,
        dst_ref=dst,
        send_sem=send_sem,
        recv_sem=recv_sem,
        device_id=device,
        device_id_type=pl.DeviceIdType.MESH,
    )
    copy.start()
    return copy


def lanes(shape):
    return lax.broadcasted_iota(jnp.int32, shape, len(shape) - 1)


def kernel(
    meta,
    table_hbm,
    refined_hbm,
    out_hbm,
    error_ref,
    worst_ref,
    tab,
    ref0,
    ref1,
    ref2,
    ref3,
    got0,
    got1,
    got2,
    got3,
    stage,
    ext,
    res,
    mid,
    sums,
    peak,
    flat,
    hz_out,
    hz_in,
    hv_out,
    hv_in,
    hc_out,
    hc_in,
    zv_out,
    zv_in,
    zm_out,
    zm_in,
    in_sem,
    out_sem,
    bulk_send,
    bulk_recv,
    halo_send,
    halo_recv,
    sum_send,
    sum_recv,
):
    ref, got = (ref0, ref1, ref2, ref3), (got0, got1, got2, got3)
    zm_here = lax.axis_index(Y) * 4 + lax.axis_index(X)
    zv_here = lax.axis_index(Z) * 2 + lax.axis_index(C)
    zm_last = zm_here == 15
    zv_last = zv_here == 7
    half = lanes((ROWS, 128)) < 64
    half_row = lanes((1, 128)) < 64
    tail = lax.rem(lanes((ROWS, 128)), 64) >= 56

    loads = [
        pltpu.make_async_copy(refined_hbm.at[t], ref[t], in_sem.at[t])
        for t in range(ITERS)
    ]
    halves = [
        pltpu.make_async_copy(
            table_hbm.at[:, pl.ds(h * 128, 128)], tab.at[h], in_sem.at[ITERS + h]
        )
        for h in range(2)
    ]
    loads[0].start()
    for load in halves:
        load.start()
    for load in loads[1:]:
        load.start()

    barrier = pltpu.get_barrier_semaphore()
    partners = [at(y, x, 0, 0) for y, x in ORDER] + [at(0, 0, z, c) for z, c in ZV_ORDER]
    partners += [beside(1, 1), beside(-1, -1)]
    for partner in partners:
        pl.semaphore_signal(
            barrier, inc=1, device_id=partner, device_id_type=pl.DeviceIdType.MESH
        )

    def order_blocks(t):
        def one(j, _):
            stage[t, j] = ref[t][meta[t, j]]
            return 0

        lax.fori_loop(1, BLK, one, 0)
        got[t][0] = ref[t][meta[t, 0]]

    def send_blocks(t):
        copies = []
        for y, x in ORDER:
            j = y * 4 + x
            copies.append(
                send(stage.at[t, j], got[t].at[j], bulk_send.at[t, j], bulk_recv.at[t, j], at(y, x, 0, 0))
            )
        return copies

    def table_to_blocks():
        def one(bv, _):
            for q in range(8):
                for h in range(2):
                    even = tab[h, pl.ds(bv * 16 + 2 * q, ROWS, stride=64), :]
                    odd = tab[h, pl.ds(bv * 16 + 2 * q + 1, ROWS, stride=64), :]
                    ext[bv * 4 + 2 * h, 0:ROWS, q * 128 : (q + 1) * 128] = jnp.where(
                        half, even, pltpu.roll(odd, 64, 1)
                    )
                    ext[bv * 4 + 2 * h + 1, 0:ROWS, q * 128 : (q + 1) * 128] = jnp.where(
                        half, pltpu.roll(even, 64, 1), odd
                    )
            return 0

        lax.fori_loop(0, 4, one, 0)

    def blocks_to_table(src, dst):
        def one(bv, _):
            for q in range(8):
                for h in range(2):
                    low = src[bv * 4 + 2 * h, 0:ROWS, q * 128 : (q + 1) * 128]
                    high = src[bv * 4 + 2 * h + 1, 0:ROWS, q * 128 : (q + 1) * 128]
                    dst[h, pl.ds(bv * 16 + 2 * q, ROWS, stride=64), :] = jnp.where(
                        half, low, pltpu.roll(high, 64, 1)
                    )
                    dst[h, pl.ds(bv * 16 + 2 * q + 1, ROWS, stride=64), :] = jnp.where(
                        half, pltpu.roll(low, 64, 1), high
                    )
            return 0

        lax.fori_loop(0, 4, one, 0)

    def send_halos(src, e):
        for l in range(BLK):
            hz_out[e, l : l + 1, :] = src[l, 0:1, :]
        for b in range(4):
            hv_out[e, b] = src[b, 0:ROWS, 0:128]
            hc_out[e, b : b + 1, :] = src[b, 0:1, 0:128]
        return [
            send(hz_out.at[e], hz_in.at[e], halo_send.at[e, 0], halo_recv.at[e, 0], beside(-1, 0)),
            send(hv_out.at[e], hv_in.at[e], halo_send.at[e, 1], halo_recv.at[e, 1], beside(0, -1)),
            send(hc_out.at[e], hc_in.at[e], halo_send.at[e, 2], halo_recv.at[e, 2], beside(-1, -1)),
        ]

    def place_halos(dst, e):
        for l in range(BLK):
            dst[l, 16:17, :] = jnp.where(zm_last, dst[l, 15:16, :], hz_in[e, l : l + 1, :])
        for b in range(4):
            own = pltpu.roll(dst[12 + b, 0:ROWS, 896:1024], 64, 1)
            dst[16 + b, 0:ROWS, 0:128] = jnp.where(zv_last, own, hv_in[e, b])
            own_row = pltpu.roll(dst[12 + b, 16:17, 896:1024], 64, 1)
            next_row = jnp.where(zm_last, hv_in[e, b, 15:16, :], hc_in[e, b : b + 1, :])
            dst[16 + b, 16:17, 0:128] = jnp.where(zv_last, own_row, next_row)

    def advance(weight):
        def one(l, _):
            ext[l, 0:ROWS, :] = ext[l, 0:ROWS, :] + weight * res[l, 0:ROWS, :]
            ext[l, 16:17, :] = ext[l, 16:17, :] + weight * res[l, 16:17, :]
            return 0

        lax.fori_loop(0, BLK, one, 0)
        for b in range(16, 20):
            ext[b, 0:ROWS, 0:128] = ext[b, 0:ROWS, 0:128] + weight * res[b, 0:ROWS, 0:128]
            ext[b, 16:17, 0:128] = ext[b, 16:17, 0:128] + weight * res[b, 16:17, 0:128]

    def interpolate():
        def along_z(l, _):
            sums[l] = ext[l, 0:ROWS, :] + ext[l, 1 : ROWS + 1, :]
            return 0

        lax.fori_loop(0, BLK, along_z, 0)
        for b in range(16, 20):
            sums[b, :, 0:128] = ext[b, 0:ROWS, 0:128] + ext[b, 1 : ROWS + 1, 0:128]

        def along_v(l, _):
            for q in range(8):
                here = sums[l, :, q * 128 : (q + 1) * 128]
                if q < 7:
                    later = sums[l, :, (q + 1) * 128 : (q + 2) * 128]
                else:
                    later = sums[l + 4, :, 0:128]
                mid[l, :, q * 128 : (q + 1) * 128] = here + pltpu.roll(
                    jnp.where(half, later, here), 64, 1
                )
            return 0

        lax.fori_loop(0, BLK, along_v, 0)

        def along_c(bv, _):
            for b in range(4):
                l = bv * 4 + b
                for q in range(8):
                    here = mid[l, :, q * 128 : (q + 1) * 128]
                    if b < 3:
                        later = pltpu.roll(mid[l + 1, :, q * 128 : (q + 1) * 128], 56, 1)
                    else:
                        later = here
                    total = here + jnp.where(tail, later, pltpu.roll(here, 120, 1))
                    sums[l, :, q * 128 : (q + 1) * 128] = total * 0.125
            return 0

        lax.fori_loop(0, 4, along_c, 0)

    def residuals(t):
        def one(l, acc):
            j = meta[t, 16 + l]
            value = got[t][jnp.maximum(j, 0)] - sums[l]
            value = jnp.where(j >= 0, value, jnp.zeros_like(value))
            res[l, 0:ROWS, :] = value
            squares, largest = jnp.zeros((8, 128), F32), jnp.zeros((8, 128), F32)
            for r in range(2):
                for q in range(8):
                    part = value[r * 8 : (r + 1) * 8, q * 128 : (q + 1) * 128]
                    squares = squares + part * part
                    largest = jnp.maximum(largest, jnp.abs(part))
            peak[t, l] = largest
            return acc + squares

        acc = lax.fori_loop(0, BLK, one, jnp.zeros((8, 128), F32))
        return jnp.sum(acc, axis=0, keepdims=True)

    row_id = lax.broadcasted_iota(jnp.int32, (8, 128), 0)

    def join(a, b):
        return jnp.where(row_id == 0, a + b, jnp.maximum(a, b))

    def gather_zv(t):
        return [
            send(zv_out.at[t], zv_in.at[t, i], sum_send.at[t, i], sum_recv.at[t, i], at(0, 0, z, c))
            for i, (z, c) in enumerate(ZV_ORDER)
        ]

    def gather_zm(t):
        return [
            send(zm_out.at[t], zm_in.at[t, i], sum_send.at[t, 7 + i], sum_recv.at[t, 7 + i], at(y, x, 0, 0))
            for i, (y, x) in enumerate(ORDER)
        ]

    def weight_of(total, t):
        whole = jnp.sum(total, axis=1, keepdims=True)
        count = jnp.full((1, 1), meta[t, 32].astype(F32) * float(ROWS * WIDE))
        return 1.0 / (1.0 + jnp.sqrt(whole / count))

    pending = []
    loads[0].wait()
    order_blocks(0)
    for load in halves:
        load.wait()
    table_to_blocks()
    for t in range(1, ITERS):
        loads[t].wait()
        order_blocks(t)
    pl.semaphore_wait(barrier, len(partners))

    halos = send_halos(ext, 0)
    bulk = {0: send_blocks(0), 1: send_blocks(1)}
    for copy in halos:
        copy.wait_recv()
    pending += halos
    place_halos(ext, 0)

    for t in range(ITERS):
        interpolate()
        for copy in bulk[t]:
            copy.wait_recv()
        squares = residuals(t)
        zv_out[t, 0:1, :] = squares
        if t == ITERS - 1:
            for s in range(ITERS):
                largest = jnp.max(jnp.max(peak[s], axis=0), axis=0, keepdims=True)
                zv_out[t, s + 1 : s + 2, :] = largest
            zv_out[t, 5:8, :] = jnp.zeros((3, 128), F32)
        else:
            zv_out[t, 1:8, :] = jnp.zeros((7, 128), F32)
        first = gather_zv(t)
        if t < ITERS - 1:
            halos = send_halos(res, t + 1)
        else:
            blocks_to_table(ext, tab)
        for copy in first:
            copy.wait_recv()
        total = zv_out[t]
        for i in range(7):
            total = join(total, zv_in[t, i])
        zm_out[t] = total
        second = gather_zm(t)
        if t + 2 < ITERS:
            bulk[t + 2] = send_blocks(t + 2)
        if t == ITERS - 1:
            blocks_to_table(res, flat)
            for s in range(ITERS):
                lane_max = jnp.max(jnp.max(peak[s], axis=1), axis=1, keepdims=True)
                eye = lax.broadcasted_iota(jnp.int32, (BLK, BLK), 0) == lanes((BLK, BLK))
                spread = jnp.where(eye, jnp.broadcast_to(lane_max, (BLK, BLK)), 0.0)
                error_ref[s : s + 1, :] = jnp.max(spread, axis=0, keepdims=True)
        for copy in second:
            copy.wait_recv()
        for i in range(15):
            total = join(total, zm_in[t, i])
        weight = weight_of(total[0:1, :], t)
        pending += first + second
        if t < ITERS - 1:
            for copy in halos:
                copy.wait_recv()
            pending += halos
            place_halos(res, t + 1)
            advance(weight)

    stores = []
    for i in range(4):
        h, rows = i % 2, pl.ds(i // 2 * 512, 512)
        tab[h, rows, :] = tab[h, rows, :] + weight * flat[h, rows, :]
        store = pltpu.make_async_copy(
            tab.at[h, rows], out_hbm.at[rows, pl.ds(h * 128, 128)], out_sem.at[i]
        )
        store.start()
        stores.append(store)
    lane_max = jnp.max(total[1:5, :], axis=1, keepdims=True)
    worst_ref[...] = jnp.broadcast_to(lane_max, (4, 128))
    for t in range(ITERS):
        pending += bulk[t]
    for copy in pending:
        copy.wait_send()
    for store in stores:
        store.wait()


def shards(table, refined, assign):
    zm_here = lax.axis_index(ZM)
    zv_here = lax.axis_index(ZV)
    me_y, me_x = zm_here // 4, zm_here % 4
    device = zm_here * 8 + zv_here
    span = jnp.arange(16, dtype=jnp.int32)
    column = lax.dynamic_index_in_dim(assign.reshape(ITERS, 16, 8, 16), zv_here, 2, False)
    mine = jnp.sum(jnp.where((span == zm_here)[None, :, None], column, 0), axis=1)
    home = mine >> 7
    partner = ((me_y + span // 4) % 4) * 4 + (me_x + span % 4) % 4
    slots = jnp.sum(
        jnp.where(home[:, None, :] == partner[None, :, None], span[None, None, :], 0), axis=2
    )
    offset = ((me_y - span // 4) % 4) * 4 + (me_x - span % 4) % 4
    held = column[:, :, :, None] == device * BLK + span
    source = jnp.max(jnp.where(held, offset[None, :, None, None], -1), axis=(1, 2))
    count = jnp.sum((assign >= 0).astype(jnp.int32), axis=(1, 2))
    meta = jnp.concatenate(
        [slots, source, jnp.broadcast_to(count[:, None], (ITERS, META - 32))], axis=1
    )

    depth, width, chan = table.shape
    any_space = pl.BlockSpec(memory_space=pl.ANY)
    vmem = pl.BlockSpec(memory_space=pltpu.VMEM)
    dma = pltpu.SemaphoreType.DMA
    flat_table = (depth * width, chan)
    table_out, errors, worst = pl.pallas_call(
        kernel,
        out_shape=(
            jax.ShapeDtypeStruct(flat_table, F32),
            jax.ShapeDtypeStruct((ITERS, BLK), F32),
            jax.ShapeDtypeStruct((ITERS, 128), F32),
        ),
        in_specs=[pl.BlockSpec(memory_space=pltpu.SMEM), any_space, any_space],
        out_specs=(any_space, vmem, vmem),
        scratch_shapes=[
            pltpu.VMEM((2, depth * width, 128), F32),
            *[pltpu.VMEM((BLK, ROWS, WIDE), F32)] * (2 * ITERS),
            pltpu.VMEM((ITERS, BLK, ROWS, WIDE), F32),
            pltpu.VMEM((20, 24, WIDE), F32),
            pltpu.VMEM((20, 24, WIDE), F32),
            pltpu.VMEM((BLK, ROWS, WIDE), F32),
            pltpu.VMEM((20, ROWS, WIDE), F32),
            pltpu.VMEM((ITERS, BLK, 8, 128), F32),
            pltpu.VMEM((2, depth * width, 128), F32),
            pltpu.VMEM((ITERS, BLK, WIDE), F32),
            pltpu.VMEM((ITERS, BLK, WIDE), F32),
            pltpu.VMEM((ITERS, 4, ROWS, 128), F32),
            pltpu.VMEM((ITERS, 4, ROWS, 128), F32),
            pltpu.VMEM((ITERS, 8, 128), F32),
            pltpu.VMEM((ITERS, 8, 128), F32),
            pltpu.VMEM((ITERS, 8, 128), F32),
            pltpu.VMEM((ITERS, 7, 8, 128), F32),
            pltpu.VMEM((ITERS, 8, 128), F32),
            pltpu.VMEM((ITERS, 15, 8, 128), F32),
            dma((ITERS + 2,)),
            dma((4,)),
            dma((ITERS, BLK)),
            dma((ITERS, BLK)),
            dma((ITERS, 3)),
            dma((ITERS, 3)),
            dma((ITERS, 22)),
            dma((ITERS, 22)),
        ],
        compiler_params=pltpu.CompilerParams(collective_id=0, has_side_effects=True),
        name="refine",
    )(meta, table.reshape(flat_table), refined)
    return table_out.reshape(table.shape), errors, worst[:, 0]


def solution(mesh):
    split = Mesh(mesh.devices.reshape(4, 4, 4, 2), NAMES)
    in_specs = (P(ZM, ZV, None), P(None, NAMES, None, None), P())
    out_specs = (P(ZM, ZV, None), P(None, NAMES), P())
    return jax.shard_map(
        shards, mesh=split, in_specs=in_specs, out_specs=out_specs, check_vma=False
    )
```

```python
import functools

import jax
import jax.numpy as jnp
from jax import lax
from jax.experimental import pallas as pl
from jax.experimental.pallas import tpu as pltpu
from jax.sharding import Mesh
from jax.sharding import PartitionSpec as P

ITERS = 4
Y, X, Z, C = "zm_0", "zm_1", "zv_0", "zv_1"
NAMES = (Y, X, Z, C)
ZM = (Y, X)
ZV = (Z, C)
BLK = 16
ROWS = 16
WIDE = 1024
LEAD = 8
F32 = jnp.float32

ORDER = (
    (2, 2), (3, 2), (2, 3), (1, 2), (2, 1), (3, 1), (1, 3), (3, 3),
    (1, 1), (2, 0), (0, 2), (3, 0), (0, 3), (1, 0), (0, 1),
)
ZV_ORDER = ((2, 1), (2, 0), (1, 1), (3, 1), (1, 0), (3, 0), (0, 1))


def at(*steps):
    return tuple(
        lax.rem(lax.axis_index(name) + step + lax.axis_size(name), lax.axis_size(name))
        for name, step in zip(NAMES, steps, strict=True)
    )


def beside(zm_step, zv_step):
    zm = lax.rem(lax.axis_index(Y) * 4 + lax.axis_index(X) + zm_step + 16, 16)
    zv = lax.rem(lax.axis_index(Z) * 2 + lax.axis_index(C) + zv_step + 8, 8)
    return (zm // 4, lax.rem(zm, 4), zv // 2, lax.rem(zv, 2))


def send(src, dst, send_sem, recv_sem, device):
    copy = pltpu.make_async_remote_copy(
        src_ref=src,
        dst_ref=dst,
        send_sem=send_sem,
        recv_sem=recv_sem,
        device_id=device,
        device_id_type=pl.DeviceIdType.MESH,
    )
    copy.start()
    return copy


def both_ends(ref, send_sem, recv_sem):
    return pltpu.make_async_remote_copy(
        src_ref=ref,
        dst_ref=ref,
        send_sem=send_sem,
        recv_sem=recv_sem,
        device_id=at(0, 0, 0, 1),
        device_id_type=pl.DeviceIdType.MESH,
    )


def within(index):
    return jnp.minimum(jnp.maximum(index, 0), BLK - 1)


def lanes(shape):
    return lax.broadcasted_iota(jnp.int32, shape, len(shape) - 1)


def kernel(
    assign_hbm,
    table_hbm,
    refined_hbm,
    tab,
    flat,
    stats_ref,
    error_ref,
    slots,
    plan,
    meta,
    ref0,
    ref1,
    ref2,
    ref3,
    got0,
    got1,
    got2,
    got3,
    stage,
    ext,
    res,
    mean,
    mean_res,
    peak,
    hz_out,
    hz_in,
    hv_out,
    hv_in,
    hc_out,
    hc_in,
    zv_out,
    zv_in,
    zm_out,
    zm_in,
    in_sem,
    bulk_send,
    bulk_recv,
    halo_send,
    halo_recv,
    sum_send,
    sum_recv,
):
    ref, got = (ref0, ref1, ref2, ref3), (got0, got1, got2, got3)
    zm_here = lax.axis_index(Y) * 4 + lax.axis_index(X)
    zv_here = lax.axis_index(Z) * 2 + lax.axis_index(C)
    zm_last = zm_here == 15
    zv_last = zv_here == 7
    half = lanes((ROWS, 128)) < 64
    half_row = lanes((1, 128)) < 64
    tail = lax.rem(lanes((ROWS, 128)), 64) >= 56

    loads = [
        pltpu.make_async_copy(refined_hbm.at[t], ref[t], in_sem.at[t])
        for t in range(ITERS)
    ]
    halves = [
        pltpu.make_async_copy(
            table_hbm.at[:, pl.ds(h * 128, 128)], tab.at[h, pl.ds(0, 1024)], in_sem.at[ITERS + h]
        )
        for h in range(2)
    ]
    slots_load = pltpu.make_async_copy(assign_hbm, slots, in_sem.at[ITERS + 2])
    plan_load = pltpu.make_async_copy(plan, meta, in_sem.at[ITERS + 3])
    slots_load.start()
    loads[0].start()
    for load in halves:
        load.start()
    for load in loads[1:]:
        load.start()

    barrier = pltpu.get_barrier_semaphore()
    partners = [at(y, x, 0, 0) for y, x in ORDER] + [at(0, 0, z, c) for z, c in ZV_ORDER]
    partners += [beside(1, 1), beside(-1, -1)]
    for partner in partners:
        pl.semaphore_signal(
            barrier, inc=1, device_id=partner, device_id_type=pl.DeviceIdType.MESH
        )

    def make_plan():
        me_y, me_x = lax.axis_index(Y), lax.axis_index(X)
        device = zm_here * 8 + zv_here
        lane, sub = lanes((BLK, 128)), lax.broadcasted_iota(jnp.int32, (BLK, 128), 0)
        offset = ((me_y - (lane >> 5)) & 3) * 4 + ((me_x - ((lane >> 3) & 3)) & 3)
        partner = ((me_y + (lane >> 2)) & 3) * 4 + ((me_x + (lane & 3)) & 3)
        for t in range(ITERS):
            block = slots[t]
            here = jnp.where((block >> 4) == device, (block & 15).astype(F32), -1.0)
            here = jnp.max(here, axis=0, keepdims=True)
            source = jnp.where(here == sub.astype(F32), offset.astype(F32), -1.0)
            source = jnp.max(source, axis=1, keepdims=True)
            source = jnp.max(jnp.where(lane == sub, source, -1.0), axis=0, keepdims=True)
            home = jnp.where(lane == device, (block >> 7).astype(F32), 0.0)
            home = jnp.sum(home, axis=1, keepdims=True)
            slot = jnp.where(home == partner.astype(F32), sub.astype(F32), 0.0)
            slot = jnp.max(slot, axis=0, keepdims=True)
            count = jnp.sum(jnp.where(block >= 0, 1.0, 0.0), axis=0, keepdims=True)
            count = jnp.sum(count, axis=1, keepdims=True)
            plan[t : t + 1, :] = slot.astype(jnp.int32)
            plan[4 + t : 5 + t, :] = jnp.where(lane[0:1] < 16, source, count).astype(jnp.int32)

    def order_blocks(t):
        def one(j, _):
            stage[t, j] = ref[t][within(meta[t, j])]
            return 0

        lax.fori_loop(1, BLK, one, 0)
        got[t][0] = ref[t][within(meta[t, 0])]

    def table_to_blocks():
        def one(bv, _):
            for q in range(8):
                for h in range(2):
                    even = tab[h, pl.ds(bv * 16 + 2 * q, ROWS, stride=64), :]
                    odd = tab[h, pl.ds(bv * 16 + 2 * q + 1, ROWS, stride=64), :]
                    ext[bv * 4 + 2 * h, 0:ROWS, q * 128 : (q + 1) * 128] = jnp.where(
                        half, even, pltpu.roll(odd, 64, 1)
                    )
                    ext[bv * 4 + 2 * h + 1, 0:ROWS, q * 128 : (q + 1) * 128] = jnp.where(
                        half, pltpu.roll(even, 64, 1), odd
                    )
            return 0

        lax.fori_loop(0, 4, one, 0)

    def blocks_to_table(src, dst):
        def one(bv, _):
            for q in range(8):
                for h in range(2):
                    low = src[bv * 4 + 2 * h, 0:ROWS, q * 128 : (q + 1) * 128]
                    high = src[bv * 4 + 2 * h + 1, 0:ROWS, q * 128 : (q + 1) * 128]
                    dst[h, pl.ds(bv * 16 + 2 * q, ROWS, stride=64), :] = jnp.where(
                        half, low, pltpu.roll(high, 64, 1)
                    )
                    dst[h, pl.ds(bv * 16 + 2 * q + 1, ROWS, stride=64), :] = jnp.where(
                        half, pltpu.roll(low, 64, 1), high
                    )
            return 0

        lax.fori_loop(0, 4, one, 0)

    def pack_table_halos():
        for h in range(2):
            first = tab[h, pl.ds(0, ROWS, stride=64), :]
            hv_out[0, 2 * h] = first
            hv_out[0, 2 * h + 1] = pltpu.roll(first, 64, 1)
            hc_out[0, 2 * h : 2 * h + 1, :] = first[0:1]
            hc_out[0, 2 * h + 1 : 2 * h + 2, :] = pltpu.roll(first[0:1], 64, 1)

    def send_sides(e):
        return [
            send(hv_out.at[e], hv_in.at[e], halo_send.at[e, 1], halo_recv.at[e, 1], beside(0, -1)),
            send(hc_out.at[e], hc_in.at[e], halo_send.at[e, 2], halo_recv.at[e, 2], beside(-1, -1)),
        ]

    def send_table_halos():
        for h in range(2):
            send(
                table_hbm.at[pl.ds(0, 64), pl.ds(h * 128, 128)],
                tab.at[h, pl.ds(1024, 64)],
                halo_send.at[0, 0],
                halo_recv.at[0, 0],
                beside(-1, 0),
            )
        rows = both_ends(hz_in.at[0], halo_send.at[0, 0], halo_recv.at[0, 0])
        return [rows, *send_sides(0)]

    def unpack_table_halos():
        def one(bv, _):
            for q in range(8):
                for h in range(2):
                    cols = slice(q * 128, (q + 1) * 128)
                    even = tab[h, pl.ds(1024 + bv * 16 + 2 * q, 1), :]
                    odd = tab[h, pl.ds(1024 + bv * 16 + 2 * q + 1, 1), :]
                    low = jnp.where(half_row, even, pltpu.roll(odd, 64, 1))
                    high = jnp.where(half_row, pltpu.roll(even, 64, 1), odd)
                    for side, row in ((2 * h, low), (2 * h + 1, high)):
                        own = ext[bv * 4 + side, 15:16, cols]
                        ext[bv * 4 + side, 16:17, cols] = jnp.where(zm_last, own, row)
            return 0

        lax.fori_loop(0, 4, one, 0)

    def send_halos(src, e):
        for l in range(BLK):
            hz_out[e, l : l + 1, :] = src[l, 0:1, :]
        for b in range(4):
            hv_out[e, b] = src[b, 0:ROWS, 0:128]
            hc_out[e, b : b + 1, :] = src[b, 0:1, 0:128]
        return [
            send(hz_out.at[e], hz_in.at[e], halo_send.at[e, 0], halo_recv.at[e, 0], beside(-1, 0)),
            *send_sides(e),
        ]

    def place_v(dst, e):
        for b in range(4):
            own = pltpu.roll(dst[12 + b, 0:ROWS, 896:1024], 64, 1)
            dst[16 + b, 0:ROWS, 0:128] = jnp.where(zv_last, own, hv_in[e, b])

    def place_z(dst, e):
        for l in range(BLK):
            dst[l, 16:17, :] = jnp.where(zm_last, dst[l, 15:16, :], hz_in[e, l : l + 1, :])

    def place_corner(dst, e):
        for b in range(4):
            own_row = pltpu.roll(dst[12 + b, 16:17, 896:1024], 64, 1)
            next_row = jnp.where(zm_last, hv_in[e, b, 15:16, :], hc_in[e, b : b + 1, :])
            dst[16 + b, 16:17, 0:128] = jnp.where(zv_last, own_row, next_row)

    def interpolate(src, dst, top):
        def one(bv, _):
            def pair(l, q):
                cols = slice(q * 128, (q + 1) * 128)
                return src[l, top : top + 8, cols] + src[l, top + 1 : top + 9, cols]

            here = [pair(bv * 4 + b, 0) for b in range(4)]
            for q in range(8):
                if q < 7:
                    later = [pair(bv * 4 + b, q + 1) for b in range(4)]
                else:
                    later = [pair(bv * 4 + 4 + b, 0) for b in range(4)]
                both = [
                    here[b] + pltpu.roll(jnp.where(half[0:8], later[b], here[b]), 64, 1)
                    for b in range(4)
                ]
                for b in range(4):
                    beyond = pltpu.roll(both[b + 1], 56, 1) if b < 3 else both[b]
                    total = both[b] + jnp.where(tail[0:8], beyond, pltpu.roll(both[b], 120, 1))
                    dst[bv * 4 + b, top : top + 8, q * 128 : (q + 1) * 128] = total * 0.125
                here = later
            return 0

        lax.fori_loop(0, 4, one, 0)

    def fold(value, op):
        parts = [
            value[r * 8 : (r + 1) * 8, q * 128 : (q + 1) * 128]
            for r in range(2)
            for q in range(8)
        ]
        while len(parts) > 1:
            parts = [op(x, y) for x, y in zip(parts[::2], parts[1::2], strict=True)]
        return parts[0]

    def pack(values):
        row = jnp.zeros((1, 128), F32)
        for i, value in enumerate(values):
            row = jnp.where(lanes((1, 128)) == i, value, row)
        return row

    def wanted_minus(t, l):
        j = meta[4 + t, l]
        value = got[t][within(j)] - mean[l]
        return j >= 0, jnp.where(j >= 0, value, jnp.zeros_like(value))

    def first_residuals():
        def one(l, acc):
            _, value = wanted_minus(0, l)
            res[l, 0:ROWS, :] = value
            peak[0, l] = fold(jnp.abs(value), jnp.maximum)
            return acc + fold(value * value, jnp.add)

        acc = lax.fori_loop(0, BLK, one, jnp.zeros((8, 128), F32))
        zm_out[0] = pack([jnp.sum(jnp.sum(acc, axis=0, keepdims=True), axis=1, keepdims=True)])

    def products(t):
        def one(l, acc):
            live, a = wanted_minus(t, l)
            b = mean_res[l]
            b = jnp.where(live, b, jnp.zeros_like(b))
            return (
                acc[0] + fold(a * a, jnp.add),
                acc[1] + fold(a * b, jnp.add),
                acc[2] + fold(b * b, jnp.add),
            )

        zero = jnp.zeros((8, 128), F32)
        sums = lax.fori_loop(0, BLK, one, (zero, zero, zero))
        zm_out[t] = pack(
            [jnp.sum(jnp.sum(acc, axis=0, keepdims=True), axis=1, keepdims=True) for acc in sums]
        )

    def residuals(t, weight):
        scale = jnp.broadcast_to(weight, (8, 128))
        zero = jnp.zeros((8, 128), F32)

        def one(l, _):
            j = meta[4 + t, l]
            live, row = j >= 0, within(j)
            largest = []
            for r in (slice(0, 8), slice(8, 16)):
                for q in range(8):
                    c = slice(q * 128, (q + 1) * 128)
                    ext[l, r, c] = ext[l, r, c] + scale * res[l, r, c]
                    moved = mean[l, r, c] + scale * mean_res[l, r, c]
                    value = jnp.where(live, got[t][row, r, c] - moved, zero)
                    if t < ITERS - 1:
                        mean[l, r, c] = moved
                    res[l, r, c] = value
                    largest.append(jnp.abs(value))
            while len(largest) > 1:
                largest = [jnp.maximum(x, y) for x, y in zip(largest[::2], largest[1::2], strict=True)]
            peak[t, l] = largest[0]
            return 0

        lax.fori_loop(0, BLK, one, 0)

    def gather_zv(src, dst, k):
        for i, (z, c) in enumerate(ZV_ORDER):
            send(src, dst.at[i], sum_send.at[k, 0], sum_recv.at[k, 0], at(0, 0, z, c))
        return both_ends(dst, sum_send.at[k, 0], sum_recv.at[k, 0])

    def gather_zm(src, dst, k):
        for i, (y, x) in enumerate(ORDER):
            send(src, dst.at[i], sum_send.at[k, 1], sum_recv.at[k, 1], at(y, x, 0, 0))
        return both_ends(dst, sum_send.at[k, 1], sum_recv.at[k, 1])

    def weight_of(sums, t, before):
        def entry(i):
            return jnp.sum(jnp.where(lanes((1, 128)) == i, sums, 0.0), axis=1, keepdims=True)

        total = entry(0)
        if t:
            total = total - before * (2.0 * entry(1) - before * entry(2))
            total = jnp.maximum(total, 0.0)
        count = jnp.full((1, 1), meta[4 + t, 16].astype(F32) * float(ROWS * WIDE))
        return 1.0 / (1.0 + jnp.sqrt(total / count))

    sent = []

    def bulk_to(stop):
        for n in range(len(sent), min(stop, ITERS * len(ORDER))):
            t, (y, x) = n // len(ORDER), ORDER[n % len(ORDER)]
            j = y * 4 + x
            send(stage.at[t, j], got[t].at[j], bulk_send.at[t], bulk_recv.at[t], at(y, x, 0, 0))
            sent.append(n)

    def bulk(t):
        return both_ends(got[t].at[pl.ds(1, BLK - 1)], bulk_send.at[t], bulk_recv.at[t])

    scope = jax.named_scope
    pending = []
    with scope("slots"):
        slots_load.wait()
    with scope("plan"):
        make_plan()
        plan_load.start()
    with scope("load"):
        for load in halves:
            load.wait()
        pack_table_halos()
    with scope("plan_wait"):
        plan_load.wait()
    with scope("load"):
        loads[0].wait()
    with scope("order"):
        order_blocks(0)
    with scope("barrier"):
        pl.semaphore_wait(barrier, len(partners))
    with scope("bulk_start"):
        halos = send_table_halos()
        pending += halos
        bulk_to(15)
    with scope("order"):
        loads[1].wait()
        order_blocks(1)
    with scope("bulk_start"):
        bulk_to(15 + LEAD)
    with scope("relayout"):
        table_to_blocks()
    with scope("order"):
        for t in range(2, ITERS):
            loads[t].wait()
            order_blocks(t)
    with scope("halo_wait"):
        halos[1].wait_recv()
    with scope("interp"):
        place_v(ext, 0)
        interpolate(ext, mean, 0)
    with scope("halo_wait"):
        halos[0].wait_recv()
        halos[2].wait_recv()
    with scope("interp"):
        unpack_table_halos()
        place_corner(ext, 0)
        interpolate(ext, mean, 8)
    weight = None
    for t in range(ITERS):
        with scope("bulk_wait"):
            bulk(t).wait_recv()
        with scope("products"):
            if t == 0:
                first_residuals()
            else:
                products(t)
        with scope("zm_start"):
            first = gather_zm(zm_out.at[t], zm_in.at[t], t)
            pending.append(first)
        if t:
            with scope("zv_wait"):
                second.wait_recv()
                sums = zv_out[t - 1] + jnp.sum(zv_in[t - 1], axis=0)
                weight = weight_of(sums, t - 1, weight)
            with scope("residual"):
                residuals(t, weight)
        if t < ITERS - 1:
            with scope("halo_out"):
                halos = send_halos(res, t + 1)
                pending += halos
            with scope("bulk_start"):
                bulk_to(t * 15 + 30 + LEAD)
            with scope("halo_wait"):
                halos[1].wait_recv()
            with scope("interp"):
                place_v(res, t + 1)
                interpolate(res, mean_res, 0)
        else:
            with scope("max_start"):
                maxima = [
                    jnp.max(jnp.max(jnp.max(peak[s], axis=0), axis=0, keepdims=True), axis=1, keepdims=True)
                    for s in range(ITERS)
                ]
                zm_out[ITERS] = pack(maxima)
                first_max = gather_zm(zm_out.at[ITERS], zm_in.at[ITERS], ITERS)
                pending.append(first_max)
            with scope("relayout"):
                blocks_to_table(ext, tab)
        with scope("zm_wait"):
            first.wait_recv()
        with scope("zv_start"):
            zv_out[t] = zm_out[t] + jnp.sum(zm_in[t], axis=0)
            second = gather_zv(zv_out.at[t], zv_in.at[t], t)
            pending.append(second)
        if t < ITERS - 1:
            with scope("halo_wait"):
                halos[0].wait_recv()
                halos[2].wait_recv()
            with scope("interp"):
                place_z(res, t + 1)
                place_corner(res, t + 1)
                interpolate(res, mean_res, 8)
    with scope("relayout"):
        blocks_to_table(res, flat)
    with scope("max_next"):
        first_max.wait_recv()
        zv_out[ITERS] = jnp.maximum(zm_out[ITERS], jnp.max(zm_in[ITERS], axis=0))
        second_max = gather_zv(zv_out.at[ITERS], zv_in.at[ITERS], ITERS)
        pending.append(second_max)
    with scope("errors"):
        for s in range(ITERS):
            lane_max = jnp.max(jnp.max(peak[s], axis=1), axis=1, keepdims=True)
            eye = lax.broadcasted_iota(jnp.int32, (BLK, BLK), 0) == lanes((BLK, BLK))
            spread = jnp.where(eye, jnp.broadcast_to(lane_max, (BLK, BLK)), 0.0)
            error_ref[s : s + 1, :] = jnp.max(spread, axis=0, keepdims=True)
    with scope("zv_wait"):
        second.wait_recv()
        sums = zv_out[ITERS - 1] + jnp.sum(zv_in[ITERS - 1], axis=0)
        weight = weight_of(sums, ITERS - 1, weight)
        stats_ref[0:1, :] = jnp.broadcast_to(weight, (1, 128))
    with scope("max_wait"):
        second_max.wait_recv()
        stats_ref[1:2, :] = jnp.maximum(zv_out[ITERS], jnp.max(zv_in[ITERS], axis=0))
        stats_ref[2:8, :] = jnp.zeros((6, 128), F32)
    with scope("drain"):
        for copy in pending + [bulk(t) for t in range(ITERS)]:
            copy.wait_send()


def finish(tab, flat, stats, errors, out_hbm, error_ref, worst_ref, out, out_sem):
    stores = []
    for i in range(8):
        h, rows = i % 2, pl.ds(i // 2 * 256, 256)
        out[h, rows, :] = tab[h, rows, :] + stats[0:1, :] * flat[h, rows, :]
        store = pltpu.make_async_copy(
            out.at[h, rows], out_hbm.at[rows, pl.ds(h * 128, 128)], out_sem.at[i]
        )
        store.start()
        stores.append(store)
    error_ref[...] = errors[...]
    worst_ref[...] = stats[1:2, 0:ITERS]
    for store in stores:
        store.wait()


def shards(table, refined, assign):
    depth, width, chan = table.shape
    flat_table = (depth * width, chan)
    any_space = pl.BlockSpec(memory_space=pl.ANY)
    vmem = pl.BlockSpec(memory_space=pltpu.VMEM)
    dma = pltpu.SemaphoreType.DMA
    halves = (2, depth * width + width, 128)
    blocks = (BLK, ROWS, WIDE)
    tab, flat, stats, errors = pl.pallas_call(
        kernel,
        out_shape=(
            pltpu.VMEM(halves, F32),
            pltpu.VMEM((2, depth * width, 128), F32),
            pltpu.VMEM((8, 128), F32),
            pltpu.VMEM((ITERS, BLK), F32),
        ),
        in_specs=[any_space] * 3,
        out_specs=(vmem,) * 4,
        scratch_shapes=[
            pltpu.VMEM((ITERS, BLK, 128), jnp.int32),
            pltpu.VMEM((8, 128), jnp.int32),
            pltpu.SMEM((8, 128), jnp.int32),
            *[pltpu.VMEM(blocks, F32)] * (2 * ITERS),
            pltpu.VMEM((ITERS, *blocks), F32),
            pltpu.VMEM((20, 24, WIDE), F32),
            pltpu.VMEM((20, 24, WIDE), F32),
            pltpu.VMEM(blocks, F32),
            pltpu.VMEM(blocks, F32),
            pltpu.VMEM((ITERS, BLK, 8, 128), F32),
            pltpu.VMEM((ITERS, BLK, WIDE), F32),
            pltpu.VMEM((ITERS, BLK, WIDE), F32),
            pltpu.VMEM((ITERS, 4, ROWS, 128), F32),
            pltpu.VMEM((ITERS, 4, ROWS, 128), F32),
            pltpu.VMEM((ITERS, 8, 128), F32),
            pltpu.VMEM((ITERS, 8, 128), F32),
            pltpu.VMEM((ITERS + 1, 1, 128), F32),
            pltpu.VMEM((ITERS + 1, 7, 1, 128), F32),
            pltpu.VMEM((ITERS + 1, 1, 128), F32),
            pltpu.VMEM((ITERS + 1, 15, 1, 128), F32),
            dma((ITERS + 4,)),
            dma((ITERS,)),
            dma((ITERS,)),
            dma((ITERS, 3)),
            dma((ITERS, 3)),
            dma((ITERS + 1, 2)),
            dma((ITERS + 1, 2)),
        ],
        compiler_params=pltpu.CompilerParams(collective_id=0, has_side_effects=True),
        name="refine",
    )(jnp.transpose(assign, (0, 2, 1)), table.reshape(flat_table), refined)
    held = [pltpu.with_memory_space_constraint(x, pltpu.VMEM) for x in (tab, flat, stats, errors)]
    table_out, errors, worst = pl.pallas_call(
        finish,
        out_shape=(
            jax.ShapeDtypeStruct(flat_table, F32),
            jax.ShapeDtypeStruct((ITERS, BLK), F32),
            jax.ShapeDtypeStruct((1, ITERS), F32),
        ),
        in_specs=[vmem] * 4,
        out_specs=(any_space, vmem, vmem),
        scratch_shapes=[pltpu.VMEM((2, depth * width, 128), F32), dma((8,))],
        name="finish",
    )(*held)
    return table_out.reshape(table.shape), errors, worst.reshape(ITERS)


def solution(mesh):
    split = Mesh(mesh.devices.reshape(4, 4, 4, 2), NAMES)
    in_specs = (P(ZM, ZV, None), P(None, NAMES, None, None), P())
    out_specs = (P(ZM, ZV, None), P(None, NAMES), P())
    return jax.shard_map(
        shards, mesh=split, in_specs=in_specs, out_specs=out_specs, check_vma=False
    )
```

```python
import functools

import jax
import jax.numpy as jnp
from jax import lax
from jax.experimental import pallas as pl
from jax.experimental.pallas import tpu as pltpu
from jax.sharding import Mesh
from jax.sharding import PartitionSpec as P

ITERS = 4
Y, X, Z, C = "zm_0", "zm_1", "zv_0", "zv_1"
NAMES = (Y, X, Z, C)
ZM = (Y, X)
ZV = (Z, C)
BLK = 16
ROWS = 16
WIDE = 1024
LEAD = (4, 4, 4, 0)
F32 = jnp.float32

ORDER = (
    (2, 2), (3, 2), (2, 3), (1, 2), (2, 1), (3, 1), (1, 3), (3, 3),
    (1, 1), (2, 0), (0, 2), (3, 0), (0, 3), (1, 0), (0, 1),
)
ZV_ORDER = ((2, 1), (2, 0), (1, 1), (3, 1), (1, 0), (3, 0), (0, 1))
OTHERS = sorted(
    [(y, x, z, c) for y in range(4) for x in range(4) for z in range(4) for c in range(2)][1:],
    key=lambda d: (-min(d[0], 4 - d[0]) - min(d[1], 4 - d[1]) - min(d[2], 4 - d[2]) - d[3] / 2, d),
)


def at(*steps):
    return tuple(
        lax.rem(lax.axis_index(name) + step + lax.axis_size(name), lax.axis_size(name))
        for name, step in zip(NAMES, steps, strict=True)
    )


def beside(zm_step, zv_step):
    zm = lax.rem(lax.axis_index(Y) * 4 + lax.axis_index(X) + zm_step + 16, 16)
    zv = lax.rem(lax.axis_index(Z) * 2 + lax.axis_index(C) + zv_step + 8, 8)
    return (zm // 4, lax.rem(zm, 4), zv // 2, lax.rem(zv, 2))


def send(src, dst, send_sem, recv_sem, device):
    copy = pltpu.make_async_remote_copy(
        src_ref=src,
        dst_ref=dst,
        send_sem=send_sem,
        recv_sem=recv_sem,
        device_id=device,
        device_id_type=pl.DeviceIdType.MESH,
    )
    copy.start()
    return copy


def both_ends(ref, send_sem, recv_sem):
    return pltpu.make_async_remote_copy(
        src_ref=ref,
        dst_ref=ref,
        send_sem=send_sem,
        recv_sem=recv_sem,
        device_id=at(0, 0, 0, 1),
        device_id_type=pl.DeviceIdType.MESH,
    )


def within(index):
    return jnp.minimum(jnp.maximum(index, 0), BLK - 1)


def lanes(shape):
    return lax.broadcasted_iota(jnp.int32, shape, len(shape) - 1)


def kernel(
    assign_hbm,
    table_hbm,
    refined_hbm,
    tab,
    flat,
    stats_ref,
    error_ref,
    slots,
    plan,
    meta,
    ref0,
    ref1,
    ref2,
    ref3,
    got0,
    got1,
    got2,
    got3,
    stage,
    ext,
    res,
    mean,
    mean_res,
    peak,
    hz_out,
    hz_in,
    hv_out,
    hv_in,
    hc_out,
    hc_in,
    sum_out,
    all_in,
    in_sem,
    bulk_send,
    bulk_recv,
    halo_send,
    halo_recv,
    sum_send,
    sum_recv,
    entered,
):
    ref, got = (ref0, ref1, ref2, ref3), (got0, got1, got2, got3)
    zm_here = lax.axis_index(Y) * 4 + lax.axis_index(X)
    zv_here = lax.axis_index(Z) * 2 + lax.axis_index(C)
    zm_last = zm_here == 15
    zv_last = zv_here == 7
    half = lanes((ROWS, 128)) < 64
    half_row = lanes((1, 128)) < 64
    tail = lax.rem(lanes((ROWS, 128)), 64) >= 56

    loads = [
        pltpu.make_async_copy(refined_hbm.at[t], ref[t], in_sem.at[t])
        for t in range(ITERS)
    ]
    halves = [
        pltpu.make_async_copy(
            table_hbm.at[:, pl.ds(h * 128, 128)], tab.at[h, pl.ds(0, 1024)], in_sem.at[ITERS + h]
        )
        for h in range(2)
    ]
    slots_load = pltpu.make_async_copy(assign_hbm, slots, in_sem.at[ITERS + 2])
    plan_load = pltpu.make_async_copy(plan, meta, in_sem.at[ITERS + 3])
    slots_load.start()
    loads[0].start()
    for load in halves:
        load.start()
    for load in loads[1:]:
        load.start()

    barrier = pltpu.get_barrier_semaphore()
    partners = [at(y, x, 0, 0) for y, x in ORDER] + [at(0, 0, z, c) for z, c in ZV_ORDER]
    partners += [beside(1, 1), beside(-1, -1)]
    for partner in partners:
        pl.semaphore_signal(
            barrier, inc=1, device_id=partner, device_id_type=pl.DeviceIdType.MESH
        )

    def make_plan():
        me_y, me_x = lax.axis_index(Y), lax.axis_index(X)
        device = zm_here * 8 + zv_here
        lane, sub = lanes((BLK, 128)), lax.broadcasted_iota(jnp.int32, (BLK, 128), 0)
        offset = ((me_y - (lane >> 5)) & 3) * 4 + ((me_x - ((lane >> 3) & 3)) & 3)
        partner = ((me_y + (lane >> 2)) & 3) * 4 + ((me_x + (lane & 3)) & 3)
        for t in range(ITERS):
            block = slots[t]
            here = jnp.where((block >> 4) == device, (block & 15).astype(F32), -1.0)
            here = jnp.max(here, axis=0, keepdims=True)
            source = jnp.where(here == sub.astype(F32), offset.astype(F32), -1.0)
            source = jnp.max(source, axis=1, keepdims=True)
            source = jnp.max(jnp.where(lane == sub, source, -1.0), axis=0, keepdims=True)
            home = jnp.where(lane == device, (block >> 7).astype(F32), 0.0)
            home = jnp.sum(home, axis=1, keepdims=True)
            slot = jnp.where(home == partner.astype(F32), sub.astype(F32), 0.0)
            slot = jnp.max(slot, axis=0, keepdims=True)
            count = jnp.sum(jnp.where(block >= 0, 1.0, 0.0), axis=0, keepdims=True)
            count = jnp.sum(count, axis=1, keepdims=True)
            plan[t : t + 1, :] = slot.astype(jnp.int32)
            plan[4 + t : 5 + t, :] = jnp.where(lane[0:1] < 16, source, count).astype(jnp.int32)

    def order_blocks(t):
        def one(j, _):
            stage[t, j] = ref[t][within(meta[t, j])]
            return 0

        lax.fori_loop(1, BLK, one, 0)
        got[t][0] = ref[t][within(meta[t, 0])]

    def table_to_blocks():
        def one(bv, _):
            for q in range(8):
                for h in range(2):
                    even = tab[h, pl.ds(bv * 16 + 2 * q, ROWS, stride=64), :]
                    odd = tab[h, pl.ds(bv * 16 + 2 * q + 1, ROWS, stride=64), :]
                    ext[bv * 4 + 2 * h, 0:ROWS, q * 128 : (q + 1) * 128] = jnp.where(
                        half, even, pltpu.roll(odd, 64, 1)
                    )
                    ext[bv * 4 + 2 * h + 1, 0:ROWS, q * 128 : (q + 1) * 128] = jnp.where(
                        half, pltpu.roll(even, 64, 1), odd
                    )
            return 0

        lax.fori_loop(0, 4, one, 0)

    def blocks_to_table(src, dst):
        def one(bv, _):
            for q in range(8):
                for h in range(2):
                    low = src[bv * 4 + 2 * h, 0:ROWS, q * 128 : (q + 1) * 128]
                    high = src[bv * 4 + 2 * h + 1, 0:ROWS, q * 128 : (q + 1) * 128]
                    dst[h, pl.ds(bv * 16 + 2 * q, ROWS, stride=64), :] = jnp.where(
                        half, low, pltpu.roll(high, 64, 1)
                    )
                    dst[h, pl.ds(bv * 16 + 2 * q + 1, ROWS, stride=64), :] = jnp.where(
                        half, pltpu.roll(low, 64, 1), high
                    )
            return 0

        lax.fori_loop(0, 4, one, 0)

    def pack_table_halos():
        for h in range(2):
            first = tab[h, pl.ds(0, ROWS, stride=64), :]
            hv_out[0, 2 * h] = first
            hv_out[0, 2 * h + 1] = pltpu.roll(first, 64, 1)
            hc_out[0, 2 * h : 2 * h + 1, :] = first[0:1]
            hc_out[0, 2 * h + 1 : 2 * h + 2, :] = pltpu.roll(first[0:1], 64, 1)

    def send_sides(e):
        return [
            send(hv_out.at[e], hv_in.at[e], halo_send.at[e, 1], halo_recv.at[e, 1], beside(0, -1)),
            send(hc_out.at[e], hc_in.at[e], halo_send.at[e, 2], halo_recv.at[e, 2], beside(-1, -1)),
        ]

    def send_table_halos():
        for h in range(2):
            send(
                table_hbm.at[pl.ds(0, 64), pl.ds(h * 128, 128)],
                tab.at[h, pl.ds(1024, 64)],
                halo_send.at[0, 0],
                halo_recv.at[0, 0],
                beside(-1, 0),
            )
        rows = both_ends(hz_in.at[0], halo_send.at[0, 0], halo_recv.at[0, 0])
        return [rows, *send_sides(0)]

    def unpack_table_halos():
        def one(bv, _):
            for q in range(8):
                for h in range(2):
                    cols = slice(q * 128, (q + 1) * 128)
                    even = tab[h, pl.ds(1024 + bv * 16 + 2 * q, 1), :]
                    odd = tab[h, pl.ds(1024 + bv * 16 + 2 * q + 1, 1), :]
                    low = jnp.where(half_row, even, pltpu.roll(odd, 64, 1))
                    high = jnp.where(half_row, pltpu.roll(even, 64, 1), odd)
                    for side, row in ((2 * h, low), (2 * h + 1, high)):
                        own = ext[bv * 4 + side, 15:16, cols]
                        ext[bv * 4 + side, 16:17, cols] = jnp.where(zm_last, own, row)
            return 0

        lax.fori_loop(0, 4, one, 0)

    def send_halos(src, e):
        for l in range(BLK):
            hz_out[e, l : l + 1, :] = src[l, 0:1, :]
        for b in range(4):
            hv_out[e, b] = src[b, 0:ROWS, 0:128]
            hc_out[e, b : b + 1, :] = src[b, 0:1, 0:128]
        return [
            send(hz_out.at[e], hz_in.at[e], halo_send.at[e, 0], halo_recv.at[e, 0], beside(-1, 0)),
            *send_sides(e),
        ]

    def place_v(dst, e):
        for b in range(4):
            own = pltpu.roll(dst[12 + b, 0:ROWS, 896:1024], 64, 1)
            dst[16 + b, 0:ROWS, 0:128] = jnp.where(zv_last, own, hv_in[e, b])

    def place_z(dst, e):
        for l in range(BLK):
            dst[l, 16:17, :] = jnp.where(zm_last, dst[l, 15:16, :], hz_in[e, l : l + 1, :])

    def place_corner(dst, e):
        for b in range(4):
            own_row = pltpu.roll(dst[12 + b, 16:17, 896:1024], 64, 1)
            next_row = jnp.where(zm_last, hv_in[e, b, 15:16, :], hc_in[e, b : b + 1, :])
            dst[16 + b, 16:17, 0:128] = jnp.where(zv_last, own_row, next_row)

    def interpolate(src, dst, top):
        def one(bv, _):
            def pair(l, q):
                cols = slice(q * 128, (q + 1) * 128)
                return src[l, top : top + 8, cols] + src[l, top + 1 : top + 9, cols]

            here = [pair(bv * 4 + b, 0) for b in range(4)]
            for q in range(8):
                if q < 7:
                    later = [pair(bv * 4 + b, q + 1) for b in range(4)]
                else:
                    later = [pair(bv * 4 + 4 + b, 0) for b in range(4)]
                both = [
                    here[b] + pltpu.roll(jnp.where(half[0:8], later[b], here[b]), 64, 1)
                    for b in range(4)
                ]
                for b in range(4):
                    beyond = pltpu.roll(both[b + 1], 56, 1) if b < 3 else both[b]
                    total = both[b] + jnp.where(tail[0:8], beyond, pltpu.roll(both[b], 120, 1))
                    dst[bv * 4 + b, top : top + 8, q * 128 : (q + 1) * 128] = total * 0.125
                here = later
            return 0

        lax.fori_loop(0, 4, one, 0)

    def fold(value, op):
        parts = [
            value[r * 8 : (r + 1) * 8, q * 128 : (q + 1) * 128]
            for r in range(2)
            for q in range(8)
        ]
        while len(parts) > 1:
            parts = [op(x, y) for x, y in zip(parts[::2], parts[1::2], strict=True)]
        return parts[0]

    def pack(values):
        row = jnp.zeros((1, 128), F32)
        for i, value in enumerate(values):
            row = jnp.where(lanes((1, 128)) == i, value, row)
        return row

    def wanted_minus(t, l):
        j = meta[4 + t, l]
        value = got[t][within(j)] - mean[l]
        return j >= 0, jnp.where(j >= 0, value, jnp.zeros_like(value))

    def first_residuals():
        def one(l, acc):
            _, value = wanted_minus(0, l)
            res[l, 0:ROWS, :] = value
            peak[0, l] = fold(jnp.abs(value), jnp.maximum)
            return acc + fold(value * value, jnp.add)

        acc = lax.fori_loop(0, BLK, one, jnp.zeros((8, 128), F32))
        sum_out[0] = pack([jnp.sum(jnp.sum(acc, axis=0, keepdims=True), axis=1, keepdims=True)])

    def products(t):
        def one(l, acc):
            live, a = wanted_minus(t, l)
            b = mean_res[l]
            b = jnp.where(live, b, jnp.zeros_like(b))
            return (
                acc[0] + fold(a * a, jnp.add),
                acc[1] + fold(a * b, jnp.add),
                acc[2] + fold(b * b, jnp.add),
            )

        zero = jnp.zeros((8, 128), F32)
        sums = lax.fori_loop(0, BLK, one, (zero, zero, zero))
        sum_out[t] = pack(
            [jnp.sum(jnp.sum(acc, axis=0, keepdims=True), axis=1, keepdims=True) for acc in sums]
        )

    def residuals(t, weight):
        scale = jnp.broadcast_to(weight, (8, 128))
        zero = jnp.zeros((8, 128), F32)

        def one(l, acc):
            j = meta[4 + t, l]
            live, row = j >= 0, within(j)
            largest, squares = [], []
            for r in (slice(0, 8), slice(8, 16)):
                for q in range(8):
                    c = slice(q * 128, (q + 1) * 128)
                    ext[l, r, c] = ext[l, r, c] + scale * res[l, r, c]
                    moved = mean[l, r, c] + scale * mean_res[l, r, c]
                    value = jnp.where(live, got[t][row, r, c] - moved, zero)
                    if t < ITERS - 1:
                        mean[l, r, c] = moved
                    res[l, r, c] = value
                    largest.append(jnp.abs(value))
                    squares.append(value * value)
            while len(largest) > 1:
                largest = [jnp.maximum(x, y) for x, y in zip(largest[::2], largest[1::2], strict=True)]
                squares = [x + y for x, y in zip(squares[::2], squares[1::2], strict=True)]
            peak[t, l] = largest[0]
            return acc + squares[0] if t == ITERS - 1 else acc

        return lax.fori_loop(0, BLK, one, zero)

    def gather(t):
        for i, steps in enumerate(OTHERS):
            send(sum_out.at[t], all_in.at[t, i], sum_send.at[t], sum_recv.at[t], at(*steps))
        return both_ends(all_in.at[t], sum_send.at[t], sum_recv.at[t])

    def weight_of(sums, t, before):
        def entry(i):
            return jnp.sum(jnp.where(lanes((1, 128)) == i, sums, 0.0), axis=1, keepdims=True)

        total = entry(0)
        if before is not None:
            total = total - before * (2.0 * entry(1) - before * entry(2))
            total = jnp.maximum(total, 0.0)
        count = jnp.full((1, 1), meta[4 + t, 16].astype(F32) * float(ROWS * WIDE))
        return 1.0 / (1.0 + jnp.sqrt(total / count))

    sent = []

    def bulk_to(stop):
        for n in range(len(sent), min(stop, ITERS * len(ORDER))):
            t, (y, x) = n // len(ORDER), ORDER[n % len(ORDER)]
            j = y * 4 + x
            send(stage.at[t, j], got[t].at[j], bulk_send.at[t], bulk_recv.at[t], at(y, x, 0, 0))
            sent.append(n)

    def bulk(t):
        return both_ends(got[t].at[pl.ds(1, BLK - 1)], bulk_send.at[t], bulk_recv.at[t])

    scope = jax.named_scope
    pending = []
    with scope("slots"):
        slots_load.wait()
    with scope("plan"):
        make_plan()
        plan_load.start()
    with scope("load"):
        for load in halves:
            load.wait()
        pack_table_halos()
    with scope("plan_wait"):
        plan_load.wait()
    with scope("load"):
        loads[0].wait()
    with scope("order"):
        order_blocks(0)
    with scope("barrier"):
        pl.semaphore_wait(barrier, len(partners))
    for z, c in ZV_ORDER:
        pl.semaphore_signal(
            entered, inc=1, device_id=at(0, 0, z, c), device_id_type=pl.DeviceIdType.MESH
        )
    with scope("bulk_start"):
        halos = send_table_halos()
        pending += halos
        bulk_to(15)
    with scope("order"):
        loads[1].wait()
        order_blocks(1)
    with scope("bulk_start"):
        bulk_to(15 + LEAD[0])
    with scope("relayout"):
        table_to_blocks()
    with scope("order"):
        for t in range(2, ITERS):
            loads[t].wait()
            order_blocks(t)
    with scope("halo_wait"):
        halos[1].wait_recv()
    with scope("interp"):
        place_v(ext, 0)
        interpolate(ext, mean, 0)
    with scope("halo_wait"):
        halos[0].wait_recv()
        halos[2].wait_recv()
    with scope("interp"):
        unpack_table_halos()
        place_corner(ext, 0)
        interpolate(ext, mean, 8)
    pl.semaphore_wait(entered, len(ZV_ORDER))
    weight = None
    for t in range(ITERS - 1):
        with scope("bulk_wait"):
            bulk(t).wait_recv()
        with scope("products"):
            if t == 0:
                first_residuals()
            else:
                products(t)
        with scope("sum_start"):
            coming = gather(t)
            pending.append(coming)
        if t:
            with scope("sum_wait"):
                gone.wait_recv()
                weight = weight_of(sum_out[t - 1] + jnp.sum(all_in[t - 1], axis=0), t - 1, weight)
            with scope("residual"):
                residuals(t, weight)
        gone = coming
        with scope("halo_out"):
            halos = send_halos(res, t + 1)
            pending += halos
        with scope("bulk_start"):
            bulk_to(t * 15 + 30 + LEAD[t + 1])
        with scope("halo_wait"):
            halos[1].wait_recv()
        with scope("interp"):
            place_v(res, t + 1)
            interpolate(res, mean_res, 0)
        with scope("halo_wait"):
            halos[0].wait_recv()
            halos[2].wait_recv()
        with scope("interp"):
            place_z(res, t + 1)
            place_corner(res, t + 1)
            interpolate(res, mean_res, 8)

    t = ITERS - 1
    with scope("sum_wait"):
        gone.wait_recv()
        weight = weight_of(sum_out[t - 1] + jnp.sum(all_in[t - 1], axis=0), t - 1, weight)
    with scope("bulk_wait"):
        bulk(t).wait_recv()
    with scope("residual"):
        squares = residuals(t, weight)
    with scope("sum_start"):
        values = [jnp.sum(jnp.sum(squares, axis=0, keepdims=True), axis=1, keepdims=True)]
        for s in range(ITERS):
            largest = jnp.max(jnp.max(peak[s], axis=0), axis=0, keepdims=True)
            values.append(jnp.max(largest, axis=1, keepdims=True))
        sum_out[t] = pack(values)
        gone = gather(t)
        pending.append(gone)
    with scope("relayout"):
        blocks_to_table(ext, tab)
        blocks_to_table(res, flat)
    with scope("errors"):
        for s in range(ITERS):
            lane_max = jnp.max(jnp.max(peak[s], axis=1), axis=1, keepdims=True)
            eye = lax.broadcasted_iota(jnp.int32, (BLK, BLK), 0) == lanes((BLK, BLK))
            spread = jnp.where(eye, jnp.broadcast_to(lane_max, (BLK, BLK)), 0.0)
            error_ref[s : s + 1, :] = jnp.max(spread, axis=0, keepdims=True)
    with scope("drain"):
        for copy in pending[:-1] + [bulk(s) for s in range(ITERS)]:
            copy.wait_send()
    with scope("sum_wait"):
        gone.wait_recv()
        gone.wait_send()
    with scope("final"):
        sums = sum_out[t] + jnp.sum(all_in[t], axis=0)
        weight = weight_of(sums, t, None)
        stats_ref[0:1, :] = jnp.broadcast_to(weight, (1, 128))
        stats_ref[1:2, :] = jnp.maximum(sum_out[t], jnp.max(all_in[t], axis=0))
        stats_ref[2:8, :] = jnp.zeros((6, 128), F32)


def finish(tab, flat, stats, errors, out_hbm, error_ref, worst_ref, out, out_sem):
    stores = []
    for i in range(8):
        h, rows = i % 2, pl.ds(i // 2 * 256, 256)
        out[h, rows, :] = tab[h, rows, :] + stats[0:1, :] * flat[h, rows, :]
        store = pltpu.make_async_copy(
            out.at[h, rows], out_hbm.at[rows, pl.ds(h * 128, 128)], out_sem.at[i]
        )
        store.start()
        stores.append(store)
    error_ref[...] = errors[...]
    worst_ref[...] = stats[1:2, 1 : ITERS + 1]
    for store in stores:
        store.wait()


def shards(table, refined, assign):
    depth, width, chan = table.shape
    flat_table = (depth * width, chan)
    any_space = pl.BlockSpec(memory_space=pl.ANY)
    vmem = pl.BlockSpec(memory_space=pltpu.VMEM)
    dma = pltpu.SemaphoreType.DMA
    halves = (2, depth * width + width, 128)
    blocks = (BLK, ROWS, WIDE)
    tab, flat, stats, errors = pl.pallas_call(
        kernel,
        out_shape=(
            pltpu.VMEM(halves, F32),
            pltpu.VMEM((2, depth * width, 128), F32),
            pltpu.VMEM((8, 128), F32),
            pltpu.VMEM((ITERS, BLK), F32),
        ),
        in_specs=[any_space] * 3,
        out_specs=(vmem,) * 4,
        scratch_shapes=[
            pltpu.VMEM((ITERS, BLK, 128), jnp.int32),
            pltpu.VMEM((8, 128), jnp.int32),
            pltpu.SMEM((8, 128), jnp.int32),
            *[pltpu.VMEM(blocks, F32)] * (2 * ITERS),
            pltpu.VMEM((ITERS, *blocks), F32),
            pltpu.VMEM((20, 24, WIDE), F32),
            pltpu.VMEM((20, 24, WIDE), F32),
            pltpu.VMEM(blocks, F32),
            pltpu.VMEM(blocks, F32),
            pltpu.VMEM((ITERS, BLK, 8, 128), F32),
            pltpu.VMEM((ITERS, BLK, WIDE), F32),
            pltpu.VMEM((ITERS, BLK, WIDE), F32),
            pltpu.VMEM((ITERS, 4, ROWS, 128), F32),
            pltpu.VMEM((ITERS, 4, ROWS, 128), F32),
            pltpu.VMEM((ITERS, 8, 128), F32),
            pltpu.VMEM((ITERS, 8, 128), F32),
            pltpu.VMEM((ITERS, 1, 128), F32),
            pltpu.VMEM((ITERS, len(OTHERS), 1, 128), F32),
            dma((ITERS + 4,)),
            dma((ITERS,)),
            dma((ITERS,)),
            dma((ITERS, 3)),
            dma((ITERS, 3)),
            dma((ITERS,)),
            dma((ITERS,)),
            pltpu.SemaphoreType.REGULAR,
        ],
        compiler_params=pltpu.CompilerParams(collective_id=0, has_side_effects=True),
        name="refine",
    )(jnp.transpose(assign, (0, 2, 1)), table.reshape(flat_table), refined)
    held = [pltpu.with_memory_space_constraint(x, pltpu.VMEM) for x in (tab, flat, stats, errors)]
    table_out, errors, worst = pl.pallas_call(
        finish,
        out_shape=(
            jax.ShapeDtypeStruct(flat_table, F32),
            jax.ShapeDtypeStruct((ITERS, BLK), F32),
            jax.ShapeDtypeStruct((1, ITERS), F32),
        ),
        in_specs=[vmem] * 4,
        out_specs=(any_space, vmem, vmem),
        scratch_shapes=[pltpu.VMEM((2, depth * width, 128), F32), dma((8,))],
        name="finish",
    )(*held)
    return table_out.reshape(table.shape), errors, worst.reshape(ITERS)


def solution(mesh):
    split = Mesh(mesh.devices.reshape(4, 4, 4, 2), NAMES)
    in_specs = (P(ZM, ZV, None), P(None, NAMES, None, None), P())
    out_specs = (P(ZM, ZV, None), P(None, NAMES), P())
    return jax.shard_map(
        shards, mesh=split, in_specs=in_specs, out_specs=out_specs, check_vma=False
    )
```

```python
import functools

import jax
import jax.numpy as jnp
from jax import lax
from jax.experimental import pallas as pl
from jax.experimental.pallas import tpu as pltpu
from jax.sharding import Mesh
from jax.sharding import PartitionSpec as P

ITERS = 4
Y, X, Z, C = "zm_0", "zm_1", "zv_0", "zv_1"
NAMES = (Y, X, Z, C)
ZM = (Y, X)
ZV = (Z, C)
BLK = 16
ROWS = 16
WIDE = 1024
TWO_STAGES = (True, True, True, False)
LEAD = (3, 3, 3, 0)
F32 = jnp.float32

ORDER = (
    (2, 2), (3, 2), (2, 3), (1, 2), (2, 1), (3, 1), (1, 3), (3, 3),
    (1, 1), (2, 0), (0, 2), (3, 0), (0, 3), (1, 0), (0, 1),
)
ZV_ORDER = ((2, 1), (2, 0), (1, 1), (3, 1), (1, 0), (3, 0), (0, 1))
OTHERS = sorted(
    [(y, x, z, c) for y in range(4) for x in range(4) for z in range(4) for c in range(2)][1:],
    key=lambda d: (-min(d[0], 4 - d[0]) - min(d[1], 4 - d[1]) - min(d[2], 4 - d[2]) - d[3] / 2, d),
)


def at(*steps):
    return tuple(
        lax.rem(lax.axis_index(name) + step + lax.axis_size(name), lax.axis_size(name))
        for name, step in zip(NAMES, steps, strict=True)
    )


def beside(zm_step, zv_step):
    zm = lax.rem(lax.axis_index(Y) * 4 + lax.axis_index(X) + zm_step + 16, 16)
    zv = lax.rem(lax.axis_index(Z) * 2 + lax.axis_index(C) + zv_step + 8, 8)
    return (zm // 4, lax.rem(zm, 4), zv // 2, lax.rem(zv, 2))


def send(src, dst, send_sem, recv_sem, device):
    copy = pltpu.make_async_remote_copy(
        src_ref=src,
        dst_ref=dst,
        send_sem=send_sem,
        recv_sem=recv_sem,
        device_id=device,
        device_id_type=pl.DeviceIdType.MESH,
    )
    copy.start()
    return copy


def both_ends(ref, send_sem, recv_sem):
    return pltpu.make_async_remote_copy(
        src_ref=ref,
        dst_ref=ref,
        send_sem=send_sem,
        recv_sem=recv_sem,
        device_id=at(0, 0, 0, 1),
        device_id_type=pl.DeviceIdType.MESH,
    )


def within(index):
    return jnp.minimum(jnp.maximum(index, 0), BLK - 1)


def lanes(shape):
    return lax.broadcasted_iota(jnp.int32, shape, len(shape) - 1)


def kernel(
    assign_hbm,
    table_hbm,
    refined_hbm,
    tab,
    flat,
    stats_ref,
    error_ref,
    slots,
    plan,
    meta,
    ref0,
    ref1,
    ref2,
    ref3,
    got0,
    got1,
    got2,
    got3,
    stage,
    ext,
    res,
    mean,
    mean_res,
    peak,
    hz_out,
    hz_in,
    hv_out,
    hv_in,
    hc_out,
    hc_in,
    sum_out,
    all_in,
    zm_in,
    zv_out,
    zv_in,
    in_sem,
    bulk_send,
    bulk_recv,
    halo_send,
    halo_recv,
    sum_send,
    sum_recv,
    line_send,
    line_recv,
    entered,
):
    ref, got = (ref0, ref1, ref2, ref3), (got0, got1, got2, got3)
    zm_here = lax.axis_index(Y) * 4 + lax.axis_index(X)
    zv_here = lax.axis_index(Z) * 2 + lax.axis_index(C)
    zm_last = zm_here == 15
    zv_last = zv_here == 7
    half = lanes((ROWS, 128)) < 64
    half_row = lanes((1, 128)) < 64
    tail = lax.rem(lanes((ROWS, 128)), 64) >= 56

    loads = [
        pltpu.make_async_copy(refined_hbm.at[t], ref[t], in_sem.at[t])
        for t in range(ITERS)
    ]
    halves = [
        pltpu.make_async_copy(
            table_hbm.at[:, pl.ds(h * 128, 128)], tab.at[h, pl.ds(0, 1024)], in_sem.at[ITERS + h]
        )
        for h in range(2)
    ]
    slots_load = pltpu.make_async_copy(assign_hbm, slots, in_sem.at[ITERS + 2])
    plan_load = pltpu.make_async_copy(plan, meta, in_sem.at[ITERS + 3])
    slots_load.start()
    loads[0].start()
    for load in halves:
        load.start()
    for load in loads[1:]:
        load.start()

    barrier = pltpu.get_barrier_semaphore()
    partners = [at(y, x, 0, 0) for y, x in ORDER] + [at(0, 0, z, c) for z, c in ZV_ORDER]
    partners += [beside(1, 1), beside(-1, -1)]
    for partner in partners:
        pl.semaphore_signal(
            barrier, inc=1, device_id=partner, device_id_type=pl.DeviceIdType.MESH
        )

    def make_plan():
        me_y, me_x = lax.axis_index(Y), lax.axis_index(X)
        device = zm_here * 8 + zv_here
        lane, sub = lanes((BLK, 128)), lax.broadcasted_iota(jnp.int32, (BLK, 128), 0)
        offset = ((me_y - (lane >> 5)) & 3) * 4 + ((me_x - ((lane >> 3) & 3)) & 3)
        partner = ((me_y + (lane >> 2)) & 3) * 4 + ((me_x + (lane & 3)) & 3)
        for t in range(ITERS):
            block = slots[t]
            here = jnp.where((block >> 4) == device, (block & 15).astype(F32), -1.0)
            here = jnp.max(here, axis=0, keepdims=True)
            source = jnp.where(here == sub.astype(F32), offset.astype(F32), -1.0)
            source = jnp.max(source, axis=1, keepdims=True)
            source = jnp.max(jnp.where(lane == sub, source, -1.0), axis=0, keepdims=True)
            home = jnp.where(lane == device, (block >> 7).astype(F32), 0.0)
            home = jnp.sum(home, axis=1, keepdims=True)
            slot = jnp.where(home == partner.astype(F32), sub.astype(F32), 0.0)
            slot = jnp.max(slot, axis=0, keepdims=True)
            count = jnp.sum(jnp.where(block >= 0, 1.0, 0.0), axis=0, keepdims=True)
            count = jnp.sum(count, axis=1, keepdims=True)
            plan[t : t + 1, :] = slot.astype(jnp.int32)
            plan[4 + t : 5 + t, :] = jnp.where(lane[0:1] < 16, source, count).astype(jnp.int32)

    def order_blocks(t):
        def one(j, _):
            stage[t, j] = ref[t][within(meta[t, j])]
            return 0

        lax.fori_loop(1, BLK, one, 0)
        got[t][0] = ref[t][within(meta[t, 0])]

    def table_to_blocks():
        def one(bv, _):
            for q in range(8):
                for h in range(2):
                    even = tab[h, pl.ds(bv * 16 + 2 * q, ROWS, stride=64), :]
                    odd = tab[h, pl.ds(bv * 16 + 2 * q + 1, ROWS, stride=64), :]
                    ext[bv * 4 + 2 * h, 0:ROWS, q * 128 : (q + 1) * 128] = jnp.where(
                        half, even, pltpu.roll(odd, 64, 1)
                    )
                    ext[bv * 4 + 2 * h + 1, 0:ROWS, q * 128 : (q + 1) * 128] = jnp.where(
                        half, pltpu.roll(even, 64, 1), odd
                    )
            return 0

        lax.fori_loop(0, 4, one, 0)

    def blocks_to_table(src, dst):
        def one(bv, _):
            for q in range(8):
                for h in range(2):
                    low = src[bv * 4 + 2 * h, 0:ROWS, q * 128 : (q + 1) * 128]
                    high = src[bv * 4 + 2 * h + 1, 0:ROWS, q * 128 : (q + 1) * 128]
                    dst[h, pl.ds(bv * 16 + 2 * q, ROWS, stride=64), :] = jnp.where(
                        half, low, pltpu.roll(high, 64, 1)
                    )
                    dst[h, pl.ds(bv * 16 + 2 * q + 1, ROWS, stride=64), :] = jnp.where(
                        half, pltpu.roll(low, 64, 1), high
                    )
            return 0

        lax.fori_loop(0, 4, one, 0)

    def pack_table_halos():
        for h in range(2):
            first = tab[h, pl.ds(0, ROWS, stride=64), :]
            hv_out[0, 2 * h] = first
            hv_out[0, 2 * h + 1] = pltpu.roll(first, 64, 1)
            hc_out[0, 2 * h : 2 * h + 1, :] = first[0:1]
            hc_out[0, 2 * h + 1 : 2 * h + 2, :] = pltpu.roll(first[0:1], 64, 1)

    def send_sides(e):
        return [
            send(hv_out.at[e], hv_in.at[e], halo_send.at[e, 1], halo_recv.at[e, 1], beside(0, -1)),
            send(hc_out.at[e], hc_in.at[e], halo_send.at[e, 2], halo_recv.at[e, 2], beside(-1, -1)),
        ]

    def send_table_halos():
        for h in range(2):
            send(
                table_hbm.at[pl.ds(0, 64), pl.ds(h * 128, 128)],
                tab.at[h, pl.ds(1024, 64)],
                halo_send.at[0, 0],
                halo_recv.at[0, 0],
                beside(-1, 0),
            )
        rows = both_ends(hz_in.at[0], halo_send.at[0, 0], halo_recv.at[0, 0])
        return [rows, *send_sides(0)]

    def unpack_table_halos():
        def one(bv, _):
            for q in range(8):
                for h in range(2):
                    cols = slice(q * 128, (q + 1) * 128)
                    even = tab[h, pl.ds(1024 + bv * 16 + 2 * q, 1), :]
                    odd = tab[h, pl.ds(1024 + bv * 16 + 2 * q + 1, 1), :]
                    low = jnp.where(half_row, even, pltpu.roll(odd, 64, 1))
                    high = jnp.where(half_row, pltpu.roll(even, 64, 1), odd)
                    for side, row in ((2 * h, low), (2 * h + 1, high)):
                        own = ext[bv * 4 + side, 15:16, cols]
                        ext[bv * 4 + side, 16:17, cols] = jnp.where(zm_last, own, row)
            return 0

        lax.fori_loop(0, 4, one, 0)

    def send_halos(src, e):
        for l in range(BLK):
            hz_out[e, l : l + 1, :] = src[l, 0:1, :]
        for b in range(4):
            hv_out[e, b] = src[b, 0:ROWS, 0:128]
            hc_out[e, b : b + 1, :] = src[b, 0:1, 0:128]
        return [
            send(hz_out.at[e], hz_in.at[e], halo_send.at[e, 0], halo_recv.at[e, 0], beside(-1, 0)),
            *send_sides(e),
        ]

    def place_v(dst, e):
        for b in range(4):
            own = pltpu.roll(dst[12 + b, 0:ROWS, 896:1024], 64, 1)
            dst[16 + b, 0:ROWS, 0:128] = jnp.where(zv_last, own, hv_in[e, b])

    def place_z(dst, e):
        for l in range(BLK):
            dst[l, 16:17, :] = jnp.where(zm_last, dst[l, 15:16, :], hz_in[e, l : l + 1, :])

    def place_corner(dst, e):
        for b in range(4):
            own_row = pltpu.roll(dst[12 + b, 16:17, 896:1024], 64, 1)
            next_row = jnp.where(zm_last, hv_in[e, b, 15:16, :], hc_in[e, b : b + 1, :])
            dst[16 + b, 16:17, 0:128] = jnp.where(zv_last, own_row, next_row)

    def interpolate(src, dst, top):
        def one(bv, _):
            def pair(l, q):
                cols = slice(q * 128, (q + 1) * 128)
                return src[l, top : top + 8, cols] + src[l, top + 1 : top + 9, cols]

            here = [pair(bv * 4 + b, 0) for b in range(4)]
            for q in range(8):
                if q < 7:
                    later = [pair(bv * 4 + b, q + 1) for b in range(4)]
                else:
                    later = [pair(bv * 4 + 4 + b, 0) for b in range(4)]
                both = [
                    here[b] + pltpu.roll(jnp.where(half[0:8], later[b], here[b]), 64, 1)
                    for b in range(4)
                ]
                for b in range(4):
                    beyond = pltpu.roll(both[b + 1], 56, 1) if b < 3 else both[b]
                    total = both[b] + jnp.where(tail[0:8], beyond, pltpu.roll(both[b], 120, 1))
                    dst[bv * 4 + b, top : top + 8, q * 128 : (q + 1) * 128] = total * 0.125
                here = later
            return 0

        lax.fori_loop(0, 4, one, 0)

    def fold(value, op):
        parts = [
            value[r * 8 : (r + 1) * 8, q * 128 : (q + 1) * 128]
            for r in range(2)
            for q in range(8)
        ]
        while len(parts) > 1:
            parts = [op(x, y) for x, y in zip(parts[::2], parts[1::2], strict=True)]
        return parts[0]

    def pack(values):
        row = jnp.zeros((1, 128), F32)
        for i, value in enumerate(values):
            row = jnp.where(lanes((1, 128)) == i, value, row)
        return row

    def wanted_minus(t, l):
        j = meta[4 + t, l]
        value = got[t][within(j)] - mean[l]
        return j >= 0, jnp.where(j >= 0, value, jnp.zeros_like(value))

    def first_residuals():
        def one(l, acc):
            _, value = wanted_minus(0, l)
            res[l, 0:ROWS, :] = value
            peak[0, l] = fold(jnp.abs(value), jnp.maximum)
            return acc + fold(value * value, jnp.add)

        acc = lax.fori_loop(0, BLK, one, jnp.zeros((8, 128), F32))
        sum_out[0] = pack([jnp.sum(jnp.sum(acc, axis=0, keepdims=True), axis=1, keepdims=True)])

    def products(t):
        def one(l, acc):
            live, a = wanted_minus(t, l)
            b = mean_res[l]
            b = jnp.where(live, b, jnp.zeros_like(b))
            return (
                acc[0] + fold(a * a, jnp.add),
                acc[1] + fold(a * b, jnp.add),
                acc[2] + fold(b * b, jnp.add),
            )

        zero = jnp.zeros((8, 128), F32)
        sums = lax.fori_loop(0, BLK, one, (zero, zero, zero))
        sum_out[t] = pack(
            [jnp.sum(jnp.sum(acc, axis=0, keepdims=True), axis=1, keepdims=True) for acc in sums]
        )

    def residuals(t, weight):
        scale = jnp.broadcast_to(weight, (8, 128))
        zero = jnp.zeros((8, 128), F32)

        def one(l, acc):
            j = meta[4 + t, l]
            live, row = j >= 0, within(j)
            largest, squares = [], []
            for r in (slice(0, 8), slice(8, 16)):
                for q in range(8):
                    c = slice(q * 128, (q + 1) * 128)
                    ext[l, r, c] = ext[l, r, c] + scale * res[l, r, c]
                    moved = mean[l, r, c] + scale * mean_res[l, r, c]
                    value = jnp.where(live, got[t][row, r, c] - moved, zero)
                    if t < ITERS - 1:
                        mean[l, r, c] = moved
                    res[l, r, c] = value
                    largest.append(jnp.abs(value))
                    squares.append(value * value)
            while len(largest) > 1:
                largest = [jnp.maximum(x, y) for x, y in zip(largest[::2], largest[1::2], strict=True)]
                squares = [x + y for x, y in zip(squares[::2], squares[1::2], strict=True)]
            peak[t, l] = largest[0]
            return acc + squares[0] if t == ITERS - 1 else acc

        return lax.fori_loop(0, BLK, one, zero)

    def gather(t):
        for i, steps in enumerate(OTHERS):
            send(sum_out.at[t], all_in.at[t, i], sum_send.at[t], sum_recv.at[t], at(*steps))
        return both_ends(all_in.at[t], sum_send.at[t], sum_recv.at[t])

    def gather_zm(t):
        for i, (y, x) in enumerate(ORDER):
            send(sum_out.at[t], zm_in.at[t, i], sum_send.at[t], sum_recv.at[t], at(y, x, 0, 0))
        return both_ends(zm_in.at[t], sum_send.at[t], sum_recv.at[t])

    def gather_zv(t):
        for i, (z, c) in enumerate(ZV_ORDER):
            send(zv_out.at[t], zv_in.at[t, i], line_send.at[t], line_recv.at[t], at(0, 0, z, c))
        return both_ends(zv_in.at[t], line_send.at[t], line_recv.at[t])

    def sums_of(t):
        if TWO_STAGES[t]:
            return zv_out[t] + jnp.sum(zv_in[t], axis=0)
        return sum_out[t] + jnp.sum(all_in[t], axis=0)

    def weight_of(sums, t, before):
        def entry(i):
            return jnp.sum(jnp.where(lanes((1, 128)) == i, sums, 0.0), axis=1, keepdims=True)

        total = entry(0)
        if before is not None:
            total = total - before * (2.0 * entry(1) - before * entry(2))
            total = jnp.maximum(total, 0.0)
        count = jnp.full((1, 1), meta[4 + t, 16].astype(F32) * float(ROWS * WIDE))
        return 1.0 / (1.0 + jnp.sqrt(total / count))

    sent = []

    def bulk_to(stop):
        for n in range(len(sent), min(stop, ITERS * len(ORDER))):
            t, (y, x) = n // len(ORDER), ORDER[n % len(ORDER)]
            j = y * 4 + x
            send(stage.at[t, j], got[t].at[j], bulk_send.at[t], bulk_recv.at[t], at(y, x, 0, 0))
            sent.append(n)

    def bulk(t):
        return both_ends(got[t].at[pl.ds(1, BLK - 1)], bulk_send.at[t], bulk_recv.at[t])

    scope = jax.named_scope
    pending = []
    with scope("slots"):
        slots_load.wait()
    with scope("plan"):
        make_plan()
        plan_load.start()
    with scope("load"):
        for load in halves:
            load.wait()
        pack_table_halos()
    with scope("plan_wait"):
        plan_load.wait()
    with scope("load"):
        loads[0].wait()
    with scope("order"):
        order_blocks(0)
    with scope("barrier"):
        pl.semaphore_wait(barrier, len(partners))
    for z, c in ZV_ORDER:
        pl.semaphore_signal(
            entered, inc=1, device_id=at(0, 0, z, c), device_id_type=pl.DeviceIdType.MESH
        )
    with scope("bulk_start"):
        halos = send_table_halos()
        pending += halos
        bulk_to(15)
    with scope("order"):
        loads[1].wait()
        order_blocks(1)
    with scope("bulk_start"):
        bulk_to(15 + LEAD[0])
    with scope("relayout"):
        table_to_blocks()
    with scope("order"):
        for t in range(2, ITERS):
            loads[t].wait()
            order_blocks(t)
    with scope("halo_wait"):
        halos[1].wait_recv()
    with scope("interp"):
        place_v(ext, 0)
        interpolate(ext, mean, 0)
    with scope("halo_wait"):
        halos[0].wait_recv()
        halos[2].wait_recv()
    with scope("interp"):
        unpack_table_halos()
        place_corner(ext, 0)
        interpolate(ext, mean, 8)
    pl.semaphore_wait(entered, len(ZV_ORDER))
    weight = None
    for t in range(ITERS - 1):
        with scope("bulk_wait"):
            bulk(t).wait_recv()
        with scope("products"):
            if t == 0:
                first_residuals()
            else:
                products(t)
        with scope("sum_start"):
            coming = gather_zm(t) if TWO_STAGES[t] else gather(t)
            pending.append(coming)
        if t:
            with scope("sum_wait"):
                gone.wait_recv()
                weight = weight_of(sums_of(t - 1), t - 1, weight)
            with scope("residual"):
                residuals(t, weight)
        gone = coming
        with scope("halo_out"):
            halos = send_halos(res, t + 1)
            pending += halos
        with scope("bulk_start"):
            bulk_to(t * 15 + 30 + LEAD[t + 1])
        with scope("halo_wait"):
            halos[1].wait_recv()
        with scope("interp"):
            place_v(res, t + 1)
            interpolate(res, mean_res, 0)
        if TWO_STAGES[t]:
            with scope("zm_wait"):
                gone.wait_recv()
                zv_out[t] = sum_out[t] + jnp.sum(zm_in[t], axis=0)
                gone = gather_zv(t)
                pending.append(gone)
        with scope("halo_wait"):
            halos[0].wait_recv()
            halos[2].wait_recv()
        with scope("interp"):
            place_z(res, t + 1)
            place_corner(res, t + 1)
            interpolate(res, mean_res, 8)

    t = ITERS - 1
    with scope("sum_wait"):
        gone.wait_recv()
        weight = weight_of(sums_of(t - 1), t - 1, weight)
    with scope("bulk_wait"):
        bulk(t).wait_recv()
    with scope("residual"):
        squares = residuals(t, weight)
    with scope("sum_start"):
        values = [jnp.sum(jnp.sum(squares, axis=0, keepdims=True), axis=1, keepdims=True)]
        for s in range(ITERS):
            largest = jnp.max(jnp.max(peak[s], axis=0), axis=0, keepdims=True)
            values.append(jnp.max(largest, axis=1, keepdims=True))
        sum_out[t] = pack(values)
        gone = gather(t)
        pending.append(gone)
    with scope("relayout"):
        blocks_to_table(ext, tab)
        blocks_to_table(res, flat)
    with scope("errors"):
        for s in range(ITERS):
            lane_max = jnp.max(jnp.max(peak[s], axis=1), axis=1, keepdims=True)
            eye = lax.broadcasted_iota(jnp.int32, (BLK, BLK), 0) == lanes((BLK, BLK))
            spread = jnp.where(eye, jnp.broadcast_to(lane_max, (BLK, BLK)), 0.0)
            error_ref[s : s + 1, :] = jnp.max(spread, axis=0, keepdims=True)
    with scope("drain"):
        for copy in pending[:-1] + [bulk(s) for s in range(ITERS)]:
            copy.wait_send()
    with scope("sum_wait"):
        gone.wait_recv()
        gone.wait_send()
    with scope("final"):
        weight = weight_of(sums_of(t), t, None)
        stats_ref[0:1, :] = jnp.broadcast_to(weight, (1, 128))
        stats_ref[1:2, :] = jnp.maximum(sum_out[t], jnp.max(all_in[t], axis=0))
        stats_ref[2:8, :] = jnp.zeros((6, 128), F32)


def finish(tab, flat, stats, errors, out_hbm, error_ref, worst_ref, out, out_sem):
    stores = []
    for i in range(8):
        h, rows = i % 2, pl.ds(i // 2 * 256, 256)
        out[h, rows, :] = tab[h, rows, :] + stats[0:1, :] * flat[h, rows, :]
        store = pltpu.make_async_copy(
            out.at[h, rows], out_hbm.at[rows, pl.ds(h * 128, 128)], out_sem.at[i]
        )
        store.start()
        stores.append(store)
    error_ref[...] = errors[...]
    worst_ref[...] = stats[1:2, 1 : ITERS + 1]
    for store in stores:
        store.wait()


def shards(table, refined, assign):
    depth, width, chan = table.shape
    flat_table = (depth * width, chan)
    any_space = pl.BlockSpec(memory_space=pl.ANY)
    vmem = pl.BlockSpec(memory_space=pltpu.VMEM)
    dma = pltpu.SemaphoreType.DMA
    halves = (2, depth * width + width, 128)
    blocks = (BLK, ROWS, WIDE)
    tab, flat, stats, errors = pl.pallas_call(
        kernel,
        out_shape=(
            pltpu.VMEM(halves, F32),
            pltpu.VMEM((2, depth * width, 128), F32),
            pltpu.VMEM((8, 128), F32),
            pltpu.VMEM((ITERS, BLK), F32),
        ),
        in_specs=[any_space] * 3,
        out_specs=(vmem,) * 4,
        scratch_shapes=[
            pltpu.VMEM((ITERS, BLK, 128), jnp.int32),
            pltpu.VMEM((8, 128), jnp.int32),
            pltpu.SMEM((8, 128), jnp.int32),
            *[pltpu.VMEM(blocks, F32)] * (2 * ITERS),
            pltpu.VMEM((ITERS, *blocks), F32),
            pltpu.VMEM((20, 24, WIDE), F32),
            pltpu.VMEM((20, 24, WIDE), F32),
            pltpu.VMEM(blocks, F32),
            pltpu.VMEM(blocks, F32),
            pltpu.VMEM((ITERS, BLK, 8, 128), F32),
            pltpu.VMEM((ITERS, BLK, WIDE), F32),
            pltpu.VMEM((ITERS, BLK, WIDE), F32),
            pltpu.VMEM((ITERS, 4, ROWS, 128), F32),
            pltpu.VMEM((ITERS, 4, ROWS, 128), F32),
            pltpu.VMEM((ITERS, 8, 128), F32),
            pltpu.VMEM((ITERS, 8, 128), F32),
            pltpu.VMEM((ITERS, 1, 128), F32),
            pltpu.VMEM((ITERS, len(OTHERS), 1, 128), F32),
            pltpu.VMEM((ITERS, len(ORDER), 1, 128), F32),
            pltpu.VMEM((ITERS, 1, 128), F32),
            pltpu.VMEM((ITERS, len(ZV_ORDER), 1, 128), F32),
            dma((ITERS + 4,)),
            dma((ITERS,)),
            dma((ITERS,)),
            dma((ITERS, 3)),
            dma((ITERS, 3)),
            dma((ITERS,)),
            dma((ITERS,)),
            dma((ITERS,)),
            dma((ITERS,)),
            pltpu.SemaphoreType.REGULAR,
        ],
        compiler_params=pltpu.CompilerParams(collective_id=0, has_side_effects=True),
        name="refine",
    )(jnp.transpose(assign, (0, 2, 1)), table.reshape(flat_table), refined)
    held = [pltpu.with_memory_space_constraint(x, pltpu.VMEM) for x in (tab, flat, stats, errors)]
    table_out, errors, worst = pl.pallas_call(
        finish,
        out_shape=(
            jax.ShapeDtypeStruct(flat_table, F32),
            jax.ShapeDtypeStruct((ITERS, BLK), F32),
            jax.ShapeDtypeStruct((1, ITERS), F32),
        ),
        in_specs=[vmem] * 4,
        out_specs=(any_space, vmem, vmem),
        scratch_shapes=[pltpu.VMEM((2, depth * width, 128), F32), dma((8,))],
        name="finish",
    )(*held)
    return table_out.reshape(table.shape), errors, worst.reshape(ITERS)


def solution(mesh):
    split = Mesh(mesh.devices.reshape(4, 4, 4, 2), NAMES)
    in_specs = (P(ZM, ZV, None), P(None, NAMES, None, None), P())
    out_specs = (P(ZM, ZV, None), P(None, NAMES), P())
    return jax.shard_map(
        shards, mesh=split, in_specs=in_specs, out_specs=out_specs, check_vma=False
    )
```

```python
import functools

import jax
import jax.numpy as jnp
from jax import lax
from jax.experimental import pallas as pl
from jax.experimental.pallas import tpu as pltpu
from jax.sharding import Mesh
from jax.sharding import PartitionSpec as P

ITERS = 4
Y, X, Z, C = "zm_0", "zm_1", "zv_0", "zv_1"
NAMES = (Y, X, Z, C)
ZM = (Y, X)
ZV = (Z, C)
BLK = 16
ROWS = 16
WIDE = 1024
TWO_STAGES = (True, True, True, False)
LEAD = (3, 3, 3, 0)
F32 = jnp.float32

ORDER = (
    (2, 2), (3, 2), (2, 3), (1, 2), (2, 1), (3, 1), (1, 3), (3, 3),
    (1, 1), (2, 0), (0, 2), (3, 0), (0, 3), (1, 0), (0, 1),
)
ZV_ORDER = ((2, 1), (2, 0), (1, 1), (3, 1), (1, 0), (3, 0), (0, 1))
OTHERS = sorted(
    [(y, x, z, c) for y in range(4) for x in range(4) for z in range(4) for c in range(2)][1:],
    key=lambda d: (-min(d[0], 4 - d[0]) - min(d[1], 4 - d[1]) - min(d[2], 4 - d[2]) - d[3] / 2, d),
)


def at(*steps):
    return tuple(
        lax.rem(lax.axis_index(name) + step + lax.axis_size(name), lax.axis_size(name))
        for name, step in zip(NAMES, steps, strict=True)
    )


def beside(zm_step, zv_step):
    zm = lax.rem(lax.axis_index(Y) * 4 + lax.axis_index(X) + zm_step + 16, 16)
    zv = lax.rem(lax.axis_index(Z) * 2 + lax.axis_index(C) + zv_step + 8, 8)
    return (zm // 4, lax.rem(zm, 4), zv // 2, lax.rem(zv, 2))


def send(src, dst, send_sem, recv_sem, device):
    copy = pltpu.make_async_remote_copy(
        src_ref=src,
        dst_ref=dst,
        send_sem=send_sem,
        recv_sem=recv_sem,
        device_id=device,
        device_id_type=pl.DeviceIdType.MESH,
    )
    copy.start()
    return copy


def both_ends(ref, send_sem, recv_sem):
    return pltpu.make_async_remote_copy(
        src_ref=ref,
        dst_ref=ref,
        send_sem=send_sem,
        recv_sem=recv_sem,
        device_id=at(0, 0, 0, 1),
        device_id_type=pl.DeviceIdType.MESH,
    )


def within(index):
    return jnp.minimum(jnp.maximum(index, 0), BLK - 1)


def lanes(shape):
    return lax.broadcasted_iota(jnp.int32, shape, len(shape) - 1)


def kernel(
    assign_hbm,
    table_hbm,
    refined_hbm,
    tab,
    flat,
    stats_ref,
    error_ref,
    slots,
    plan,
    meta,
    ref0,
    ref1,
    ref2,
    ref3,
    got0,
    got1,
    got2,
    got3,
    stage,
    ext,
    res,
    mean,
    mean_res,
    peak,
    hz_out,
    hz_in,
    hv_out,
    hv_in,
    hc_out,
    hc_in,
    sum_out,
    all_in,
    zm_in,
    zv_out,
    zv_in,
    in_sem,
    bulk_send,
    bulk_recv,
    halo_send,
    halo_recv,
    sum_send,
    sum_recv,
    line_send,
    line_recv,
    entered,
):
    ref, got = (ref0, ref1, ref2, ref3), (got0, got1, got2, got3)
    zm_here = lax.axis_index(Y) * 4 + lax.axis_index(X)
    zv_here = lax.axis_index(Z) * 2 + lax.axis_index(C)
    zm_last = zm_here == 15
    zv_last = zv_here == 7
    half = lanes((ROWS, 128)) < 64
    half_row = lanes((1, 128)) < 64
    tail = lax.rem(lanes((ROWS, 128)), 64) >= 56

    loads = [
        pltpu.make_async_copy(refined_hbm.at[t], ref[t], in_sem.at[t])
        for t in range(ITERS)
    ]
    halves = [
        pltpu.make_async_copy(
            table_hbm.at[:, pl.ds(h * 128, 128)], tab.at[h, pl.ds(0, 1024)], in_sem.at[ITERS + h]
        )
        for h in range(2)
    ]
    slots_load = pltpu.make_async_copy(assign_hbm, slots, in_sem.at[ITERS + 2])
    plan_load = pltpu.make_async_copy(plan, meta, in_sem.at[ITERS + 3])
    slots_load.start()
    loads[0].start()
    for load in halves:
        load.start()
    for load in loads[1:]:
        load.start()

    barrier = pltpu.get_barrier_semaphore()
    partners = [at(y, x, 0, 0) for y, x in ORDER] + [at(0, 0, z, c) for z, c in ZV_ORDER]
    partners += [beside(1, 1), beside(-1, -1)]
    for partner in partners:
        pl.semaphore_signal(
            barrier, inc=1, device_id=partner, device_id_type=pl.DeviceIdType.MESH
        )

    def make_plan():
        me_y, me_x = lax.axis_index(Y), lax.axis_index(X)
        device = zm_here * 8 + zv_here
        lane, sub = lanes((BLK, 128)), lax.broadcasted_iota(jnp.int32, (BLK, 128), 0)
        offset = ((me_y - (lane >> 5)) & 3) * 4 + ((me_x - ((lane >> 3) & 3)) & 3)
        partner = ((me_y + (lane >> 2)) & 3) * 4 + ((me_x + (lane & 3)) & 3)
        for t in range(ITERS):
            block = slots[t]
            here = jnp.where((block >> 4) == device, (block & 15).astype(F32), -1.0)
            here = jnp.max(here, axis=0, keepdims=True)
            source = jnp.where(here == sub.astype(F32), offset.astype(F32), -1.0)
            source = jnp.max(source, axis=1, keepdims=True)
            source = jnp.max(jnp.where(lane == sub, source, -1.0), axis=0, keepdims=True)
            home = jnp.where(lane == device, (block >> 7).astype(F32), 0.0)
            home = jnp.sum(home, axis=1, keepdims=True)
            slot = jnp.where(home == partner.astype(F32), sub.astype(F32), 0.0)
            slot = jnp.max(slot, axis=0, keepdims=True)
            count = jnp.sum(jnp.where(block >= 0, 1.0, 0.0), axis=0, keepdims=True)
            count = jnp.sum(count, axis=1, keepdims=True)
            plan[t : t + 1, :] = slot.astype(jnp.int32)
            plan[4 + t : 5 + t, :] = jnp.where(lane[0:1] < 16, source, count).astype(jnp.int32)

    def order_blocks(t):
        def one(j, _):
            stage[t, j] = ref[t][within(meta[t, j])]
            return 0

        lax.fori_loop(1, BLK, one, 0)
        got[t][0] = ref[t][within(meta[t, 0])]

    def table_to_blocks():
        def one(bv, _):
            for q in range(8):
                for h in range(2):
                    even = tab[h, pl.ds(bv * 16 + 2 * q, ROWS, stride=64), :]
                    odd = tab[h, pl.ds(bv * 16 + 2 * q + 1, ROWS, stride=64), :]
                    ext[bv * 4 + 2 * h, 0:ROWS, q * 128 : (q + 1) * 128] = jnp.where(
                        half, even, pltpu.roll(odd, 64, 1)
                    )
                    ext[bv * 4 + 2 * h + 1, 0:ROWS, q * 128 : (q + 1) * 128] = jnp.where(
                        half, pltpu.roll(even, 64, 1), odd
                    )
            return 0

        lax.fori_loop(0, 4, one, 0)

    def blocks_to_table(src, dst):
        def one(bv, _):
            for q in range(8):
                for h in range(2):
                    low = src[bv * 4 + 2 * h, 0:ROWS, q * 128 : (q + 1) * 128]
                    high = src[bv * 4 + 2 * h + 1, 0:ROWS, q * 128 : (q + 1) * 128]
                    dst[h, pl.ds(bv * 16 + 2 * q, ROWS, stride=64), :] = jnp.where(
                        half, low, pltpu.roll(high, 64, 1)
                    )
                    dst[h, pl.ds(bv * 16 + 2 * q + 1, ROWS, stride=64), :] = jnp.where(
                        half, pltpu.roll(low, 64, 1), high
                    )
            return 0

        lax.fori_loop(0, 4, one, 0)

    def pack_table_halos():
        for h in range(2):
            first = tab[h, pl.ds(0, ROWS, stride=64), :]
            hv_out[0, 2 * h] = first
            hv_out[0, 2 * h + 1] = pltpu.roll(first, 64, 1)
            hc_out[0, 2 * h : 2 * h + 1, :] = first[0:1]
            hc_out[0, 2 * h + 1 : 2 * h + 2, :] = pltpu.roll(first[0:1], 64, 1)

    def send_sides(e):
        return [
            send(hv_out.at[e], hv_in.at[e], halo_send.at[e, 1], halo_recv.at[e, 1], beside(0, -1)),
            send(hc_out.at[e], hc_in.at[e], halo_send.at[e, 2], halo_recv.at[e, 2], beside(-1, -1)),
        ]

    def send_table_halos():
        for h in range(2):
            send(
                table_hbm.at[pl.ds(0, 64), pl.ds(h * 128, 128)],
                tab.at[h, pl.ds(1024, 64)],
                halo_send.at[0, 0],
                halo_recv.at[0, 0],
                beside(-1, 0),
            )
        rows = both_ends(hz_in.at[0], halo_send.at[0, 0], halo_recv.at[0, 0])
        return [rows, *send_sides(0)]

    def unpack_table_halos():
        def one(bv, _):
            for q in range(8):
                for h in range(2):
                    cols = slice(q * 128, (q + 1) * 128)
                    even = tab[h, pl.ds(1024 + bv * 16 + 2 * q, 1), :]
                    odd = tab[h, pl.ds(1024 + bv * 16 + 2 * q + 1, 1), :]
                    low = jnp.where(half_row, even, pltpu.roll(odd, 64, 1))
                    high = jnp.where(half_row, pltpu.roll(even, 64, 1), odd)
                    for side, row in ((2 * h, low), (2 * h + 1, high)):
                        own = ext[bv * 4 + side, 15:16, cols]
                        ext[bv * 4 + side, 16:17, cols] = jnp.where(zm_last, own, row)
            return 0

        lax.fori_loop(0, 4, one, 0)

    def send_halos(src, e):
        for l in range(BLK):
            hz_out[e, l : l + 1, :] = src[l, 0:1, :]
        for b in range(4):
            hv_out[e, b] = src[b, 0:ROWS, 0:128]
            hc_out[e, b : b + 1, :] = src[b, 0:1, 0:128]
        return [
            send(hz_out.at[e], hz_in.at[e], halo_send.at[e, 0], halo_recv.at[e, 0], beside(-1, 0)),
            *send_sides(e),
        ]

    def place_v(dst, e):
        for b in range(4):
            own = pltpu.roll(dst[12 + b, 0:ROWS, 896:1024], 64, 1)
            dst[16 + b, 0:ROWS, 0:128] = jnp.where(zv_last, own, hv_in[e, b])

    def place_z(dst, e):
        for l in range(BLK):
            dst[l, 16:17, :] = jnp.where(zm_last, dst[l, 15:16, :], hz_in[e, l : l + 1, :])

    def place_corner(dst, e):
        for b in range(4):
            own_row = pltpu.roll(dst[12 + b, 16:17, 896:1024], 64, 1)
            next_row = jnp.where(zm_last, hv_in[e, b, 15:16, :], hc_in[e, b : b + 1, :])
            dst[16 + b, 16:17, 0:128] = jnp.where(zv_last, own_row, next_row)

    def interpolate(src, dst, top):
        def one(bv, _):
            def pair(l, q):
                cols = slice(q * 128, (q + 1) * 128)
                return src[l, top : top + 8, cols] + src[l, top + 1 : top + 9, cols]

            here = [pair(bv * 4 + b, 0) for b in range(4)]
            for q in range(8):
                if q < 7:
                    later = [pair(bv * 4 + b, q + 1) for b in range(4)]
                else:
                    later = [pair(bv * 4 + 4 + b, 0) for b in range(4)]
                both = [
                    here[b] + pltpu.roll(jnp.where(half[0:8], later[b], here[b]), 64, 1)
                    for b in range(4)
                ]
                for b in range(4):
                    beyond = pltpu.roll(both[b + 1], 56, 1) if b < 3 else both[b]
                    total = both[b] + jnp.where(tail[0:8], beyond, pltpu.roll(both[b], 120, 1))
                    dst[bv * 4 + b, top : top + 8, q * 128 : (q + 1) * 128] = total * 0.125
                here = later
            return 0

        lax.fori_loop(0, 4, one, 0)

    def fold(value, op):
        parts = [
            value[r * 8 : (r + 1) * 8, q * 128 : (q + 1) * 128]
            for r in range(2)
            for q in range(8)
        ]
        while len(parts) > 1:
            parts = [op(x, y) for x, y in zip(parts[::2], parts[1::2], strict=True)]
        return parts[0]

    def pack(values):
        row = jnp.zeros((1, 128), F32)
        for i, value in enumerate(values):
            row = jnp.where(lanes((1, 128)) == i, value, row)
        return row

    def wanted_minus(t, l):
        j = meta[4 + t, l]
        value = got[t][within(j)] - mean[l]
        return j >= 0, jnp.where(j >= 0, value, jnp.zeros_like(value))

    def first_residuals():
        def one(l, acc):
            _, value = wanted_minus(0, l)
            res[l, 0:ROWS, :] = value
            peak[0, l] = fold(jnp.abs(value), jnp.maximum)
            return acc + fold(value * value, jnp.add)

        acc = lax.fori_loop(0, BLK, one, jnp.zeros((8, 128), F32))
        sum_out[0] = pack([jnp.sum(jnp.sum(acc, axis=0, keepdims=True), axis=1, keepdims=True)])

    def products(t):
        def one(l, acc):
            live, a = wanted_minus(t, l)
            b = mean_res[l]
            b = jnp.where(live, b, jnp.zeros_like(b))
            return (
                acc[0] + fold(a * a, jnp.add),
                acc[1] + fold(a * b, jnp.add),
                acc[2] + fold(b * b, jnp.add),
            )

        zero = jnp.zeros((8, 128), F32)
        sums = lax.fori_loop(0, BLK, one, (zero, zero, zero))
        sum_out[t] = pack(
            [jnp.sum(jnp.sum(acc, axis=0, keepdims=True), axis=1, keepdims=True) for acc in sums]
        )

    def residuals(t, weight):
        scale = jnp.broadcast_to(weight, (8, 128))
        zero = jnp.zeros((8, 128), F32)

        def one(l, acc):
            j = meta[4 + t, l]
            live, row = j >= 0, within(j)
            largest, squares = [], []
            for r in (slice(0, 8), slice(8, 16)):
                for q in range(8):
                    c = slice(q * 128, (q + 1) * 128)
                    ext[l, r, c] = ext[l, r, c] + scale * res[l, r, c]
                    moved = mean[l, r, c] + scale * mean_res[l, r, c]
                    value = jnp.where(live, got[t][row, r, c] - moved, zero)
                    if t < ITERS - 1:
                        mean[l, r, c] = moved
                    res[l, r, c] = value
                    largest.append(jnp.abs(value))
                    squares.append(value * value)
            while len(largest) > 1:
                largest = [jnp.maximum(x, y) for x, y in zip(largest[::2], largest[1::2], strict=True)]
                squares = [x + y for x, y in zip(squares[::2], squares[1::2], strict=True)]
            peak[t, l] = largest[0]
            return acc + squares[0] if t == ITERS - 1 else acc

        return lax.fori_loop(0, BLK, one, zero)

    def gather(t):
        for i, steps in enumerate(OTHERS):
            send(sum_out.at[t], all_in.at[t, i], sum_send.at[t], sum_recv.at[t], at(*steps))
        return both_ends(all_in.at[t], sum_send.at[t], sum_recv.at[t])

    def gather_zm(t):
        for i, (y, x) in enumerate(ORDER):
            send(sum_out.at[t], zm_in.at[t, i], sum_send.at[t], sum_recv.at[t], at(y, x, 0, 0))
        return both_ends(zm_in.at[t], sum_send.at[t], sum_recv.at[t])

    def gather_zv(t):
        for i, (z, c) in enumerate(ZV_ORDER):
            send(zv_out.at[t], zv_in.at[t, i], line_send.at[t], line_recv.at[t], at(0, 0, z, c))
        return both_ends(zv_in.at[t], line_send.at[t], line_recv.at[t])

    def sums_of(t):
        if TWO_STAGES[t]:
            return zv_out[t] + jnp.sum(zv_in[t], axis=0)
        return sum_out[t] + jnp.sum(all_in[t], axis=0)

    def weight_of(sums, t, before):
        def entry(i):
            return jnp.sum(jnp.where(lanes((1, 128)) == i, sums, 0.0), axis=1, keepdims=True)

        total = entry(0)
        if before is not None:
            total = total - before * (2.0 * entry(1) - before * entry(2))
            total = jnp.maximum(total, 0.0)
        count = jnp.full((1, 1), meta[4 + t, 16].astype(F32) * float(ROWS * WIDE))
        return 1.0 / (1.0 + jnp.sqrt(total / count))

    sent = []

    def bulk_to(stop):
        for n in range(len(sent), min(stop, ITERS * len(ORDER))):
            t, (y, x) = n // len(ORDER), ORDER[n % len(ORDER)]
            j = y * 4 + x
            send(stage.at[t, j], got[t].at[j], bulk_send.at[t], bulk_recv.at[t], at(y, x, 0, 0))
            sent.append(n)

    def bulk(t):
        return both_ends(got[t].at[pl.ds(1, BLK - 1)], bulk_send.at[t], bulk_recv.at[t])

    scope = jax.named_scope
    pending = []
    with scope("slots"):
        slots_load.wait()
    with scope("plan"):
        make_plan()
        plan_load.start()
    with scope("load"):
        for load in halves:
            load.wait()
        pack_table_halos()
    with scope("plan_wait"):
        plan_load.wait()
    with scope("load"):
        loads[0].wait()
    with scope("order"):
        order_blocks(0)
    with scope("barrier"):
        pl.semaphore_wait(barrier, len(partners))
    for z, c in ZV_ORDER:
        pl.semaphore_signal(
            entered, inc=1, device_id=at(0, 0, z, c), device_id_type=pl.DeviceIdType.MESH
        )
    with scope("bulk_start"):
        halos = send_table_halos()
        pending += halos
        bulk_to(15)
    with scope("order"):
        loads[1].wait()
        order_blocks(1)
    with scope("bulk_start"):
        bulk_to(15 + LEAD[0])
    with scope("relayout"):
        table_to_blocks()
    with scope("order"):
        for t in range(2, ITERS):
            loads[t].wait()
            order_blocks(t)
    with scope("halo_wait"):
        halos[1].wait_recv()
    with scope("interp"):
        place_v(ext, 0)
        interpolate(ext, mean, 0)
    with scope("halo_wait"):
        halos[0].wait_recv()
        halos[2].wait_recv()
    with scope("interp"):
        unpack_table_halos()
        place_corner(ext, 0)
        interpolate(ext, mean, 8)
    pl.semaphore_wait(entered, len(ZV_ORDER))
    weight = None
    for t in range(ITERS - 1):
        with scope("bulk_wait"):
            bulk(t).wait_recv()
        with scope("products"):
            if t == 0:
                first_residuals()
            else:
                products(t)
        with scope("sum_start"):
            coming = gather_zm(t) if TWO_STAGES[t] else gather(t)
            pending.append(coming)
        if t:
            with scope("sum_wait"):
                gone.wait_recv()
                weight = weight_of(sums_of(t - 1), t - 1, weight)
            with scope("residual"):
                residuals(t, weight)
        gone = coming
        with scope("halo_out"):
            halos = send_halos(res, t + 1)
            pending += halos
        with scope("bulk_start"):
            bulk_to(t * 15 + 30 + LEAD[t + 1])
        with scope("halo_wait"):
            halos[1].wait_recv()
        with scope("interp"):
            place_v(res, t + 1)
            interpolate(res, mean_res, 0)
        if TWO_STAGES[t]:
            with scope("zm_wait"):
                gone.wait_recv()
                zv_out[t] = sum_out[t] + jnp.sum(zm_in[t], axis=0)
                gone = gather_zv(t)
                pending.append(gone)
        with scope("halo_wait"):
            halos[0].wait_recv()
            halos[2].wait_recv()
        with scope("interp"):
            place_z(res, t + 1)
            place_corner(res, t + 1)
            interpolate(res, mean_res, 8)

    t = ITERS - 1
    with scope("sum_wait"):
        gone.wait_recv()
        weight = weight_of(sums_of(t - 1), t - 1, weight)
    with scope("bulk_wait"):
        bulk(t).wait_recv()
    with scope("residual"):
        squares = residuals(t, weight)
    with scope("sum_start"):
        values = [jnp.sum(jnp.sum(squares, axis=0, keepdims=True), axis=1, keepdims=True)]
        for s in range(ITERS):
            largest = jnp.max(jnp.max(peak[s], axis=0), axis=0, keepdims=True)
            values.append(jnp.max(largest, axis=1, keepdims=True))
        sum_out[t] = pack(values)
        gone = gather(t)
        pending.append(gone)
    with scope("relayout"):
        blocks_to_table(ext, tab)
        blocks_to_table(res, flat)
    with scope("errors"):
        for s in range(ITERS):
            lane_max = jnp.max(jnp.max(peak[s], axis=1), axis=1, keepdims=True)
            eye = lax.broadcasted_iota(jnp.int32, (BLK, BLK), 0) == lanes((BLK, BLK))
            spread = jnp.where(eye, jnp.broadcast_to(lane_max, (BLK, BLK)), 0.0)
            error_ref[s : s + 1, :] = jnp.max(spread, axis=0, keepdims=True)
    with scope("drain"):
        for copy in pending[:-1] + [bulk(s) for s in range(ITERS)]:
            copy.wait_send()
    with scope("sum_wait"):
        gone.wait_recv()
        gone.wait_send()
    with scope("final"):
        weight = weight_of(sums_of(t), t, None)
        stats_ref[0:1, :] = jnp.broadcast_to(weight, (1, 128))
        stats_ref[1:2, :] = jnp.maximum(sum_out[t], jnp.max(all_in[t], axis=0))
        stats_ref[2:8, :] = jnp.zeros((6, 128), F32)


def finish(tab, flat, stats, errors, out_hbm, error_hbm, worst_hbm, out, worst, out_sem):
    worst[...] = stats[1:2, 1 : ITERS + 1]
    stores = []
    for i in range(8):
        h, rows = i % 2, pl.ds(i // 2 * 256, 256)
        out[h, rows, :] = tab[h, rows, :] + stats[0:1, :] * flat[h, rows, :]
        store = pltpu.make_async_copy(
            out.at[h, rows], out_hbm.at[rows, pl.ds(h * 128, 128)], out_sem.at[i]
        )
        store.start()
        stores.append(store)
        if i == 0:
            stores.append(pltpu.make_async_copy(errors, error_hbm, out_sem.at[8]))
            stores.append(pltpu.make_async_copy(worst, worst_hbm, out_sem.at[9]))
            stores[1].start()
            stores[2].start()
    for store in stores:
        store.wait()


def shards(table, refined, assign):
    depth, width, chan = table.shape
    flat_table = (depth * width, chan)
    any_space = pl.BlockSpec(memory_space=pl.ANY)
    vmem = pl.BlockSpec(memory_space=pltpu.VMEM)
    dma = pltpu.SemaphoreType.DMA
    halves = (2, depth * width + width, 128)
    blocks = (BLK, ROWS, WIDE)
    tab, flat, stats, errors = pl.pallas_call(
        kernel,
        out_shape=(
            pltpu.VMEM(halves, F32),
            pltpu.VMEM((2, depth * width, 128), F32),
            pltpu.VMEM((8, 128), F32),
            pltpu.VMEM((ITERS, BLK), F32),
        ),
        in_specs=[any_space] * 3,
        out_specs=(vmem,) * 4,
        scratch_shapes=[
            pltpu.VMEM((ITERS, BLK, 128), jnp.int32),
            pltpu.VMEM((8, 128), jnp.int32),
            pltpu.SMEM((8, 128), jnp.int32),
            *[pltpu.VMEM(blocks, F32)] * (2 * ITERS),
            pltpu.VMEM((ITERS, *blocks), F32),
            pltpu.VMEM((20, 24, WIDE), F32),
            pltpu.VMEM((20, 24, WIDE), F32),
            pltpu.VMEM(blocks, F32),
            pltpu.VMEM(blocks, F32),
            pltpu.VMEM((ITERS, BLK, 8, 128), F32),
            pltpu.VMEM((ITERS, BLK, WIDE), F32),
            pltpu.VMEM((ITERS, BLK, WIDE), F32),
            pltpu.VMEM((ITERS, 4, ROWS, 128), F32),
            pltpu.VMEM((ITERS, 4, ROWS, 128), F32),
            pltpu.VMEM((ITERS, 8, 128), F32),
            pltpu.VMEM((ITERS, 8, 128), F32),
            pltpu.VMEM((ITERS, 1, 128), F32),
            pltpu.VMEM((ITERS, len(OTHERS), 1, 128), F32),
            pltpu.VMEM((ITERS, len(ORDER), 1, 128), F32),
            pltpu.VMEM((ITERS, 1, 128), F32),
            pltpu.VMEM((ITERS, len(ZV_ORDER), 1, 128), F32),
            dma((ITERS + 4,)),
            dma((ITERS,)),
            dma((ITERS,)),
            dma((ITERS, 3)),
            dma((ITERS, 3)),
            dma((ITERS,)),
            dma((ITERS,)),
            dma((ITERS,)),
            dma((ITERS,)),
            pltpu.SemaphoreType.REGULAR,
        ],
        compiler_params=pltpu.CompilerParams(collective_id=0, has_side_effects=True),
        name="refine",
    )(jnp.transpose(assign, (0, 2, 1)), table.reshape(flat_table), refined)
    held = [pltpu.with_memory_space_constraint(x, pltpu.VMEM) for x in (tab, flat, stats, errors)]
    table_out, errors, worst = pl.pallas_call(
        finish,
        out_shape=(
            jax.ShapeDtypeStruct(flat_table, F32),
            jax.ShapeDtypeStruct((ITERS, BLK), F32),
            jax.ShapeDtypeStruct((1, ITERS), F32),
        ),
        in_specs=[vmem] * 4,
        out_specs=(any_space,) * 3,
        scratch_shapes=[
            pltpu.VMEM((2, depth * width, 128), F32),
            pltpu.VMEM((1, ITERS), F32),
            dma((10,)),
        ],
        name="finish",
    )(*held)
    return table_out.reshape(table.shape), errors, worst.reshape(ITERS)


def solution(mesh):
    split = Mesh(mesh.devices.reshape(4, 4, 4, 2), NAMES)
    in_specs = (P(ZM, ZV, None), P(None, NAMES, None, None), P())
    out_specs = (P(ZM, ZV, None), P(None, NAMES), P())
    return jax.shard_map(
        shards, mesh=split, in_specs=in_specs, out_specs=out_specs, check_vma=False
    )
```

```python
import functools

import jax
import jax.numpy as jnp
from jax import lax
from jax.experimental import pallas as pl
from jax.experimental.pallas import tpu as pltpu
from jax.sharding import Mesh
from jax.sharding import PartitionSpec as P

ITERS = 4
Y, X, Z, C = "zm_0", "zm_1", "zv_0", "zv_1"
NAMES = (Y, X, Z, C)
ZM = (Y, X)
ZV = (Z, C)
BLK = 16
ROWS = 16
WIDE = 1024
TWO_STAGES = (True, True, True, False)
LEAD = (3, 3, 3, 0)
F32 = jnp.float32

ORDER = (
    (2, 2), (3, 2), (2, 3), (1, 2), (2, 1), (3, 1), (1, 3), (3, 3),
    (1, 1), (2, 0), (0, 2), (3, 0), (0, 3), (1, 0), (0, 1),
)
ZV_ORDER = ((2, 1), (2, 0), (1, 1), (3, 1), (1, 0), (3, 0), (0, 1))
OTHERS = sorted(
    [(y, x, z, c) for y in range(4) for x in range(4) for z in range(4) for c in range(2)][1:],
    key=lambda d: (-min(d[0], 4 - d[0]) - min(d[1], 4 - d[1]) - min(d[2], 4 - d[2]) - d[3] / 2, d),
)


def at(*steps):
    return tuple(
        lax.rem(lax.axis_index(name) + step + lax.axis_size(name), lax.axis_size(name))
        for name, step in zip(NAMES, steps, strict=True)
    )


def beside(zm_step, zv_step):
    zm = lax.rem(lax.axis_index(Y) * 4 + lax.axis_index(X) + zm_step + 16, 16)
    zv = lax.rem(lax.axis_index(Z) * 2 + lax.axis_index(C) + zv_step + 8, 8)
    return (zm // 4, lax.rem(zm, 4), zv // 2, lax.rem(zv, 2))


def send(src, dst, send_sem, recv_sem, device):
    copy = pltpu.make_async_remote_copy(
        src_ref=src,
        dst_ref=dst,
        send_sem=send_sem,
        recv_sem=recv_sem,
        device_id=device,
        device_id_type=pl.DeviceIdType.MESH,
    )
    copy.start()
    return copy


def both_ends(ref, send_sem, recv_sem):
    return pltpu.make_async_remote_copy(
        src_ref=ref,
        dst_ref=ref,
        send_sem=send_sem,
        recv_sem=recv_sem,
        device_id=at(0, 0, 0, 1),
        device_id_type=pl.DeviceIdType.MESH,
    )


def within(index):
    return jnp.minimum(jnp.maximum(index, 0), BLK - 1)


def lanes(shape):
    return lax.broadcasted_iota(jnp.int32, shape, len(shape) - 1)


def kernel(
    assign_hbm,
    table_hbm,
    refined_hbm,
    tab,
    flat,
    stats_ref,
    error_ref,
    slots,
    plan,
    meta,
    ref0,
    ref1,
    ref2,
    ref3,
    got0,
    got1,
    got2,
    got3,
    stage,
    ext,
    res,
    mean,
    mean_res,
    peak,
    hz_out,
    hz_in,
    hv_out,
    hv_in,
    hc_out,
    hc_in,
    sum_out,
    all_in,
    zm_in,
    zv_out,
    zv_in,
    early,
    in_sem,
    bulk_send,
    bulk_recv,
    halo_send,
    halo_recv,
    sum_send,
    sum_recv,
    line_send,
    line_recv,
    entered,
):
    ref, got = (ref0, ref1, ref2, ref3), (got0, got1, got2, got3)
    zm_here = lax.axis_index(Y) * 4 + lax.axis_index(X)
    zv_here = lax.axis_index(Z) * 2 + lax.axis_index(C)
    zm_last = zm_here == 15
    zv_last = zv_here == 7
    half = lanes((ROWS, 128)) < 64
    half_row = lanes((1, 128)) < 64
    tail = lax.rem(lanes((ROWS, 128)), 64) >= 56

    loads = [
        pltpu.make_async_copy(refined_hbm.at[t], ref[t], in_sem.at[t])
        for t in range(ITERS)
    ]
    halves = [
        pltpu.make_async_copy(
            table_hbm.at[:, pl.ds(h * 128, 128)], tab.at[h, pl.ds(0, 1024)], in_sem.at[ITERS + h]
        )
        for h in range(2)
    ]
    slots_load = pltpu.make_async_copy(assign_hbm, slots, in_sem.at[ITERS + 2])
    plan_load = pltpu.make_async_copy(plan, meta, in_sem.at[ITERS + 3])
    slots_load.start()
    loads[0].start()
    for load in halves:
        load.start()
    for load in loads[1:]:
        load.start()

    barrier = pltpu.get_barrier_semaphore()
    partners = [at(y, x, 0, 0) for y, x in ORDER] + [at(0, 0, z, c) for z, c in ZV_ORDER]
    partners += [beside(1, 1), beside(-1, -1)]
    for partner in partners:
        pl.semaphore_signal(
            barrier, inc=1, device_id=partner, device_id_type=pl.DeviceIdType.MESH
        )

    def make_plan():
        me_y, me_x = lax.axis_index(Y), lax.axis_index(X)
        device = zm_here * 8 + zv_here
        lane, sub = lanes((BLK, 128)), lax.broadcasted_iota(jnp.int32, (BLK, 128), 0)
        offset = ((me_y - (lane >> 5)) & 3) * 4 + ((me_x - ((lane >> 3) & 3)) & 3)
        partner = ((me_y + (lane >> 2)) & 3) * 4 + ((me_x + (lane & 3)) & 3)
        for t in range(ITERS):
            block = slots[t]
            here = jnp.where((block >> 4) == device, (block & 15).astype(F32), -1.0)
            here = jnp.max(here, axis=0, keepdims=True)
            source = jnp.where(here == sub.astype(F32), offset.astype(F32), -1.0)
            source = jnp.max(source, axis=1, keepdims=True)
            source = jnp.max(jnp.where(lane == sub, source, -1.0), axis=0, keepdims=True)
            home = jnp.where(lane == device, (block >> 7).astype(F32), 0.0)
            home = jnp.sum(home, axis=1, keepdims=True)
            slot = jnp.where(home == partner.astype(F32), sub.astype(F32), 0.0)
            slot = jnp.max(slot, axis=0, keepdims=True)
            count = jnp.sum(jnp.where(block >= 0, 1.0, 0.0), axis=0, keepdims=True)
            count = jnp.sum(count, axis=1, keepdims=True)
            plan[t : t + 1, :] = slot.astype(jnp.int32)
            plan[4 + t : 5 + t, :] = jnp.where(lane[0:1] < 16, source, count).astype(jnp.int32)

    def order_blocks(t):
        def one(j, _):
            stage[t, j] = ref[t][within(meta[t, j])]
            return 0

        lax.fori_loop(1, BLK, one, 0)
        got[t][0] = ref[t][within(meta[t, 0])]

    def table_to_blocks():
        def one(bv, _):
            for q in range(8):
                for h in range(2):
                    even = tab[h, pl.ds(bv * 16 + 2 * q, ROWS, stride=64), :]
                    odd = tab[h, pl.ds(bv * 16 + 2 * q + 1, ROWS, stride=64), :]
                    ext[bv * 4 + 2 * h, 0:ROWS, q * 128 : (q + 1) * 128] = jnp.where(
                        half, even, pltpu.roll(odd, 64, 1)
                    )
                    ext[bv * 4 + 2 * h + 1, 0:ROWS, q * 128 : (q + 1) * 128] = jnp.where(
                        half, pltpu.roll(even, 64, 1), odd
                    )
            return 0

        lax.fori_loop(0, 4, one, 0)

    def blocks_to_table(src, dst):
        def one(bv, _):
            for q in range(8):
                for h in range(2):
                    low = src[bv * 4 + 2 * h, 0:ROWS, q * 128 : (q + 1) * 128]
                    high = src[bv * 4 + 2 * h + 1, 0:ROWS, q * 128 : (q + 1) * 128]
                    dst[h, pl.ds(bv * 16 + 2 * q, ROWS, stride=64), :] = jnp.where(
                        half, low, pltpu.roll(high, 64, 1)
                    )
                    dst[h, pl.ds(bv * 16 + 2 * q + 1, ROWS, stride=64), :] = jnp.where(
                        half, pltpu.roll(low, 64, 1), high
                    )
            return 0

        lax.fori_loop(0, 4, one, 0)

    def pack_table_halos():
        for h in range(2):
            first = tab[h, pl.ds(0, ROWS, stride=64), :]
            hv_out[0, 2 * h] = first
            hv_out[0, 2 * h + 1] = pltpu.roll(first, 64, 1)
            hc_out[0, 2 * h : 2 * h + 1, :] = first[0:1]
            hc_out[0, 2 * h + 1 : 2 * h + 2, :] = pltpu.roll(first[0:1], 64, 1)

    def send_sides(e):
        return [
            send(hv_out.at[e], hv_in.at[e], halo_send.at[e, 1], halo_recv.at[e, 1], beside(0, -1)),
            send(hc_out.at[e], hc_in.at[e], halo_send.at[e, 2], halo_recv.at[e, 2], beside(-1, -1)),
        ]

    def send_table_halos():
        for h in range(2):
            send(
                table_hbm.at[pl.ds(0, 64), pl.ds(h * 128, 128)],
                tab.at[h, pl.ds(1024, 64)],
                halo_send.at[0, 0],
                halo_recv.at[0, 0],
                beside(-1, 0),
            )
        rows = both_ends(hz_in.at[0], halo_send.at[0, 0], halo_recv.at[0, 0])
        return [rows, *send_sides(0)]

    def unpack_table_halos():
        def one(bv, _):
            for q in range(8):
                for h in range(2):
                    cols = slice(q * 128, (q + 1) * 128)
                    even = tab[h, pl.ds(1024 + bv * 16 + 2 * q, 1), :]
                    odd = tab[h, pl.ds(1024 + bv * 16 + 2 * q + 1, 1), :]
                    low = jnp.where(half_row, even, pltpu.roll(odd, 64, 1))
                    high = jnp.where(half_row, pltpu.roll(even, 64, 1), odd)
                    for side, row in ((2 * h, low), (2 * h + 1, high)):
                        own = ext[bv * 4 + side, 15:16, cols]
                        ext[bv * 4 + side, 16:17, cols] = jnp.where(zm_last, own, row)
            return 0

        lax.fori_loop(0, 4, one, 0)

    def send_halos(src, e):
        for l in range(BLK):
            hz_out[e, l : l + 1, :] = src[l, 0:1, :]
        for b in range(4):
            hv_out[e, b] = src[b, 0:ROWS, 0:128]
            hc_out[e, b : b + 1, :] = src[b, 0:1, 0:128]
        return [
            send(hz_out.at[e], hz_in.at[e], halo_send.at[e, 0], halo_recv.at[e, 0], beside(-1, 0)),
            *send_sides(e),
        ]

    def place_v(dst, e):
        for b in range(4):
            own = pltpu.roll(dst[12 + b, 0:ROWS, 896:1024], 64, 1)
            dst[16 + b, 0:ROWS, 0:128] = jnp.where(zv_last, own, hv_in[e, b])

    def place_z(dst, e):
        for l in range(BLK):
            dst[l, 16:17, :] = jnp.where(zm_last, dst[l, 15:16, :], hz_in[e, l : l + 1, :])

    def place_corner(dst, e):
        for b in range(4):
            own_row = pltpu.roll(dst[12 + b, 16:17, 896:1024], 64, 1)
            next_row = jnp.where(zm_last, hv_in[e, b, 15:16, :], hc_in[e, b : b + 1, :])
            dst[16 + b, 16:17, 0:128] = jnp.where(zv_last, own_row, next_row)

    def interpolate(src, dst, top):
        def one(bv, _):
            def pair(l, q):
                cols = slice(q * 128, (q + 1) * 128)
                return src[l, top : top + 8, cols] + src[l, top + 1 : top + 9, cols]

            here = [pair(bv * 4 + b, 0) for b in range(4)]
            for q in range(8):
                if q < 7:
                    later = [pair(bv * 4 + b, q + 1) for b in range(4)]
                else:
                    later = [pair(bv * 4 + 4 + b, 0) for b in range(4)]
                both = [
                    here[b] + pltpu.roll(jnp.where(half[0:8], later[b], here[b]), 64, 1)
                    for b in range(4)
                ]
                for b in range(4):
                    beyond = pltpu.roll(both[b + 1], 56, 1) if b < 3 else both[b]
                    total = both[b] + jnp.where(tail[0:8], beyond, pltpu.roll(both[b], 120, 1))
                    dst[bv * 4 + b, top : top + 8, q * 128 : (q + 1) * 128] = total * 0.125
                here = later
            return 0

        lax.fori_loop(0, 4, one, 0)

    def fold(value, op):
        parts = [
            value[r * 8 : (r + 1) * 8, q * 128 : (q + 1) * 128]
            for r in range(2)
            for q in range(8)
        ]
        while len(parts) > 1:
            parts = [op(x, y) for x, y in zip(parts[::2], parts[1::2], strict=True)]
        return parts[0]

    def pack(values):
        row = jnp.zeros((1, 128), F32)
        for i, value in enumerate(values):
            row = jnp.where(lanes((1, 128)) == i, value, row)
        return row

    def wanted_minus(t, l):
        j = meta[4 + t, l]
        value = got[t][within(j)] - mean[l]
        return j >= 0, jnp.where(j >= 0, value, jnp.zeros_like(value))

    def first_residuals():
        def one(l, acc):
            _, value = wanted_minus(0, l)
            res[l, 0:ROWS, :] = value
            peak[0, l] = fold(jnp.abs(value), jnp.maximum)
            return acc + fold(value * value, jnp.add)

        acc = lax.fori_loop(0, BLK, one, jnp.zeros((8, 128), F32))
        sum_out[0] = pack([jnp.sum(jnp.sum(acc, axis=0, keepdims=True), axis=1, keepdims=True)])

    def products(t):
        def one(l, acc):
            live, a = wanted_minus(t, l)
            b = mean_res[l]
            b = jnp.where(live, b, jnp.zeros_like(b))
            return (
                acc[0] + fold(a * a, jnp.add),
                acc[1] + fold(a * b, jnp.add),
                acc[2] + fold(b * b, jnp.add),
            )

        zero = jnp.zeros((8, 128), F32)
        sums = lax.fori_loop(0, BLK, one, (zero, zero, zero))
        sum_out[t] = pack(
            [jnp.sum(jnp.sum(acc, axis=0, keepdims=True), axis=1, keepdims=True) for acc in sums]
        )

    def residuals(t, weight):
        scale = jnp.broadcast_to(weight, (8, 128))
        zero = jnp.zeros((8, 128), F32)

        def one(l, acc):
            j = meta[4 + t, l]
            live, row = j >= 0, within(j)
            largest, squares = [], []
            for r in (slice(0, 8), slice(8, 16)):
                for q in range(8):
                    c = slice(q * 128, (q + 1) * 128)
                    ext[l, r, c] = ext[l, r, c] + scale * res[l, r, c]
                    moved = mean[l, r, c] + scale * mean_res[l, r, c]
                    value = jnp.where(live, got[t][row, r, c] - moved, zero)
                    if t < ITERS - 1:
                        mean[l, r, c] = moved
                    res[l, r, c] = value
                    largest.append(jnp.abs(value))
                    squares.append(value * value)
            while len(largest) > 1:
                largest = [jnp.maximum(x, y) for x, y in zip(largest[::2], largest[1::2], strict=True)]
                squares = [x + y for x, y in zip(squares[::2], squares[1::2], strict=True)]
            peak[t, l] = largest[0]
            return acc + squares[0] if t == ITERS - 1 else acc

        return lax.fori_loop(0, BLK, one, zero)

    def gather(t):
        for i, steps in enumerate(OTHERS):
            send(sum_out.at[t], all_in.at[t, i], sum_send.at[t], sum_recv.at[t], at(*steps))
        return both_ends(all_in.at[t], sum_send.at[t], sum_recv.at[t])

    def gather_zm(t):
        for i, (y, x) in enumerate(ORDER):
            send(sum_out.at[t], zm_in.at[t, i], sum_send.at[t], sum_recv.at[t], at(y, x, 0, 0))
        return both_ends(zm_in.at[t], sum_send.at[t], sum_recv.at[t])

    def gather_zv(t):
        for i, (z, c) in enumerate(ZV_ORDER):
            send(zv_out.at[t], zv_in.at[t, i], line_send.at[t], line_recv.at[t], at(0, 0, z, c))
        return both_ends(zv_in.at[t], line_send.at[t], line_recv.at[t])

    def sums_of(t):
        if TWO_STAGES[t]:
            return zv_out[t] + jnp.sum(zv_in[t], axis=0)
        return sum_out[t] + jnp.sum(all_in[t], axis=0)

    def weight_of(sums, t, before):
        def entry(i):
            return jnp.sum(jnp.where(lanes((1, 128)) == i, sums, 0.0), axis=1, keepdims=True)

        total = entry(0)
        if before is not None:
            total = total - before * (2.0 * entry(1) - before * entry(2))
            total = jnp.maximum(total, 0.0)
        count = jnp.full((1, 1), meta[4 + t, 16].astype(F32) * float(ROWS * WIDE))
        return 1.0 / (1.0 + jnp.sqrt(total / count))

    sent = []

    def bulk_to(stop):
        for n in range(len(sent), min(stop, ITERS * len(ORDER))):
            t, (y, x) = n // len(ORDER), ORDER[n % len(ORDER)]
            j = y * 4 + x
            send(stage.at[t, j], got[t].at[j], bulk_send.at[t], bulk_recv.at[t], at(y, x, 0, 0))
            sent.append(n)

    def bulk(t):
        return both_ends(got[t].at[pl.ds(1, BLK - 1)], bulk_send.at[t], bulk_recv.at[t])

    scope = jax.named_scope
    pending = []
    with scope("slots"):
        slots_load.wait()
    with scope("plan"):
        make_plan()
        plan_load.start()
    with scope("load"):
        for load in halves:
            load.wait()
        pack_table_halos()
    with scope("plan_wait"):
        plan_load.wait()
    with scope("load"):
        loads[0].wait()
    with scope("order"):
        order_blocks(0)
    with scope("barrier"):
        pl.semaphore_wait(barrier, len(partners))
    for z, c in ZV_ORDER:
        pl.semaphore_signal(
            entered, inc=1, device_id=at(0, 0, z, c), device_id_type=pl.DeviceIdType.MESH
        )
    with scope("bulk_start"):
        halos = send_table_halos()
        pending += halos
        bulk_to(15)
    with scope("order"):
        loads[1].wait()
        order_blocks(1)
    with scope("bulk_start"):
        bulk_to(15 + LEAD[0])
    with scope("relayout"):
        table_to_blocks()
    with scope("order"):
        for t in range(2, ITERS):
            loads[t].wait()
            order_blocks(t)
    with scope("halo_wait"):
        halos[1].wait_recv()
    with scope("interp"):
        place_v(ext, 0)
        interpolate(ext, mean, 0)
    with scope("halo_wait"):
        halos[0].wait_recv()
        halos[2].wait_recv()
    with scope("interp"):
        unpack_table_halos()
        place_corner(ext, 0)
        interpolate(ext, mean, 8)
    pl.semaphore_wait(entered, len(ZV_ORDER))
    weight = None
    for t in range(ITERS - 1):
        with scope("bulk_wait"):
            bulk(t).wait_recv()
        with scope("products"):
            if t == 0:
                first_residuals()
            else:
                products(t)
        with scope("sum_start"):
            coming = gather_zm(t) if TWO_STAGES[t] else gather(t)
            pending.append(coming)
        if t:
            with scope("sum_wait"):
                gone.wait_recv()
                weight = weight_of(sums_of(t - 1), t - 1, weight)
            with scope("residual"):
                residuals(t, weight)
        gone = coming
        with scope("halo_out"):
            halos = send_halos(res, t + 1)
            pending += halos
        with scope("bulk_start"):
            bulk_to(t * 15 + 30 + LEAD[t + 1])
        with scope("halo_wait"):
            halos[1].wait_recv()
        with scope("interp"):
            place_v(res, t + 1)
            interpolate(res, mean_res, 0)
        if TWO_STAGES[t]:
            with scope("zm_wait"):
                gone.wait_recv()
                zv_out[t] = sum_out[t] + jnp.sum(zm_in[t], axis=0)
                gone = gather_zv(t)
                pending.append(gone)
        with scope("halo_wait"):
            halos[0].wait_recv()
            halos[2].wait_recv()
        with scope("interp"):
            place_z(res, t + 1)
            place_corner(res, t + 1)
            interpolate(res, mean_res, 8)

    def largest_of(s):
        largest = jnp.max(jnp.max(peak[s], axis=0), axis=0, keepdims=True)
        return jnp.max(largest, axis=1, keepdims=True)

    t = ITERS - 1
    with scope("maxima"):
        early[...] = pack([jnp.zeros((1, 1), F32), *[largest_of(s) for s in range(t)]])
    with scope("sum_wait"):
        gone.wait_recv()
        weight = weight_of(sums_of(t - 1), t - 1, weight)
    with scope("bulk_wait"):
        bulk(t).wait_recv()
    with scope("residual"):
        squares = residuals(t, weight)
    with scope("sum_start"):
        total = jnp.sum(jnp.sum(squares, axis=0, keepdims=True), axis=1, keepdims=True)
        row = jnp.where(lanes((1, 128)) == 0, total, early[...])
        sum_out[t] = jnp.where(lanes((1, 128)) == ITERS, largest_of(t), row)
        gone = gather(t)
        pending.append(gone)
    with scope("relayout"):
        blocks_to_table(ext, tab)
        blocks_to_table(res, flat)
    with scope("errors"):
        for s in range(ITERS):
            lane_max = jnp.max(jnp.max(peak[s], axis=1), axis=1, keepdims=True)
            eye = lax.broadcasted_iota(jnp.int32, (BLK, BLK), 0) == lanes((BLK, BLK))
            spread = jnp.where(eye, jnp.broadcast_to(lane_max, (BLK, BLK)), 0.0)
            error_ref[s : s + 1, :] = jnp.max(spread, axis=0, keepdims=True)
    with scope("drain"):
        for copy in pending[:-1] + [bulk(s) for s in range(ITERS)]:
            copy.wait_send()
    with scope("sum_wait"):
        gone.wait_recv()
        gone.wait_send()
    with scope("final"):
        weight = weight_of(sums_of(t), t, None)
        stats_ref[0:1, :] = jnp.broadcast_to(weight, (1, 128))
        stats_ref[1:2, :] = jnp.maximum(sum_out[t], jnp.max(all_in[t], axis=0))
        stats_ref[2:8, :] = jnp.zeros((6, 128), F32)


def finish(tab, flat, stats, errors, out_hbm, error_hbm, worst_hbm, out, worst, out_sem):
    worst[...] = stats[1:2, 1 : ITERS + 1]
    stores = []
    for i in range(8):
        h, rows = i % 2, pl.ds(i // 2 * 256, 256)
        out[h, rows, :] = tab[h, rows, :] + stats[0:1, :] * flat[h, rows, :]
        store = pltpu.make_async_copy(
            out.at[h, rows], out_hbm.at[rows, pl.ds(h * 128, 128)], out_sem.at[i]
        )
        store.start()
        stores.append(store)
        if i == 0:
            stores.append(pltpu.make_async_copy(errors, error_hbm, out_sem.at[8]))
            stores.append(pltpu.make_async_copy(worst, worst_hbm, out_sem.at[9]))
            stores[1].start()
            stores[2].start()
    for store in stores:
        store.wait()


def shards(table, refined, assign):
    depth, width, chan = table.shape
    flat_table = (depth * width, chan)
    any_space = pl.BlockSpec(memory_space=pl.ANY)
    vmem = pl.BlockSpec(memory_space=pltpu.VMEM)
    dma = pltpu.SemaphoreType.DMA
    halves = (2, depth * width + width, 128)
    blocks = (BLK, ROWS, WIDE)
    tab, flat, stats, errors = pl.pallas_call(
        kernel,
        out_shape=(
            pltpu.VMEM(halves, F32),
            pltpu.VMEM((2, depth * width, 128), F32),
            pltpu.VMEM((8, 128), F32),
            pltpu.VMEM((ITERS, BLK), F32),
        ),
        in_specs=[any_space] * 3,
        out_specs=(vmem,) * 4,
        scratch_shapes=[
            pltpu.VMEM((ITERS, BLK, 128), jnp.int32),
            pltpu.VMEM((8, 128), jnp.int32),
            pltpu.SMEM((8, 128), jnp.int32),
            *[pltpu.VMEM(blocks, F32)] * (2 * ITERS),
            pltpu.VMEM((ITERS, *blocks), F32),
            pltpu.VMEM((20, 24, WIDE), F32),
            pltpu.VMEM((20, 24, WIDE), F32),
            pltpu.VMEM(blocks, F32),
            pltpu.VMEM(blocks, F32),
            pltpu.VMEM((ITERS, BLK, 8, 128), F32),
            pltpu.VMEM((ITERS, BLK, WIDE), F32),
            pltpu.VMEM((ITERS, BLK, WIDE), F32),
            pltpu.VMEM((ITERS, 4, ROWS, 128), F32),
            pltpu.VMEM((ITERS, 4, ROWS, 128), F32),
            pltpu.VMEM((ITERS, 8, 128), F32),
            pltpu.VMEM((ITERS, 8, 128), F32),
            pltpu.VMEM((ITERS, 1, 128), F32),
            pltpu.VMEM((ITERS, len(OTHERS), 1, 128), F32),
            pltpu.VMEM((ITERS, len(ORDER), 1, 128), F32),
            pltpu.VMEM((ITERS, 1, 128), F32),
            pltpu.VMEM((ITERS, len(ZV_ORDER), 1, 128), F32),
            pltpu.VMEM((1, 128), F32),
            dma((ITERS + 4,)),
            dma((ITERS,)),
            dma((ITERS,)),
            dma((ITERS, 3)),
            dma((ITERS, 3)),
            dma((ITERS,)),
            dma((ITERS,)),
            dma((ITERS,)),
            dma((ITERS,)),
            pltpu.SemaphoreType.REGULAR,
        ],
        compiler_params=pltpu.CompilerParams(collective_id=0, has_side_effects=True),
        name="refine",
    )(jnp.transpose(assign, (0, 2, 1)), table.reshape(flat_table), refined)
    held = [pltpu.with_memory_space_constraint(x, pltpu.VMEM) for x in (tab, flat, stats, errors)]
    table_out, errors, worst = pl.pallas_call(
        finish,
        out_shape=(
            jax.ShapeDtypeStruct(flat_table, F32),
            jax.ShapeDtypeStruct((ITERS, BLK), F32),
            jax.ShapeDtypeStruct((1, ITERS), F32),
        ),
        in_specs=[vmem] * 4,
        out_specs=(any_space,) * 3,
        scratch_shapes=[
            pltpu.VMEM((2, depth * width, 128), F32),
            pltpu.VMEM((1, ITERS), F32),
            dma((10,)),
        ],
        name="finish",
    )(*held)
    return table_out.reshape(table.shape), errors, worst.reshape(ITERS)


def solution(mesh):
    split = Mesh(mesh.devices.reshape(4, 4, 4, 2), NAMES)
    in_specs = (P(ZM, ZV, None), P(None, NAMES, None, None), P())
    out_specs = (P(ZM, ZV, None), P(None, NAMES), P())
    return jax.shard_map(
        shards, mesh=split, in_specs=in_specs, out_specs=out_specs, check_vma=False
    )
```
